128 devices in a mesh: group: 4 (over z_lo, core), space: 32 (over z_hi, y, x).
Axes of the slice: x: 4, y: 4, z: 4 (z_hi: 2, z_lo: 2; z = z_hi * 2 + z_lo), core: 2. Of those that a mesh axis runs over, the one named last changes fastest.
Arguments:
- latents: bfloat16 [16, 64, 128, 256], P('group', 'space'), may hold values from -6 to 6
- first_kernel: bfloat16 [3, 3, 3, 256, 256], replicated, may hold values from -0.078125 to 0.078125
- second_kernel: bfloat16 [3, 3, 3, 256, 256], replicated, may hold values from -0.078125 to 0.078125
- upstream: bfloat16 [16, 64, 128, 256], P('group', 'space'), may hold values from -6 to 6
Outputs:
- decoded: bfloat16 [16, 64, 128, 256], P('group', 'space')
- latent_grad: bfloat16 [16, 64, 128, 256], P('group', 'space')
- first_grad: float32 [3, 3, 3, 256, 256], replicated
- second_grad: float32 [3, 3, 3, 256, 256], replicated
The draws below stay inside these ranges and needn't reach their ends.
All inputs are finite; a program needn't handle non-finite values.
Results may differ from the reference program's by a relative error of at most 0.0054.
Values may be sent and summed in bfloat16 or wider, within the bound.
No kernel may reach another device: no remote copies, remote signals or barrier semaphores. Data moves between devices by JAX's collectives and lax.ppermute only.
A program may use at most 192 MiB of HBM per device.

```python
import jax
import jax.numpy as jnp
from jax import lax

C = 256
W = 128
T_SIZE = 16
H = 64


def levels(key, extent, shards, low, top_value):
    def one(dim, blocks):
        draws = jax.random.uniform(jax.random.fold_in(jax.random.fold_in(key, 6), dim), (blocks,), jnp.float32, low / len(shards), top_value / len(shards))
        return jnp.repeat(jnp.exp(draws), extent[dim] // blocks).reshape((-1,) + (1,) * (len(extent) - dim - 1))

    level = one(*shards[0])
    for cut in shards[1:]:
        level = level * one(*cut)
    return level


def normal_values(own_key, extent, deviation, most, shards=(), kind=jnp.bfloat16):
    loudness = levels(own_key, extent, shards, -0.22, 0.18) if shards else 1.0
    result = jax.random.normal(own_key, extent, jnp.float32) * deviation * loudness
    return jnp.minimum(jnp.maximum(result, -most), most).astype(kind)


def setup_inputs(seed: int = 0) -> dict:
    splits = jax.random.split(jax.random.key(seed), 5)
    latents = normal_values(splits[0], (T_SIZE, H, W, C), 1.0, 6.0, ((0, 4), (1, 32)))
    first_kernel = normal_values(splits[1], (3, 3, 3, C, C), (27 * C) ** -0.5, 0.078125)
    second_kernel = normal_values(splits[2], (3, 3, 3, C, C), (27 * C) ** -0.5, 0.078125)
    upstream = normal_values(splits[3], (T_SIZE, H, W, C), 1.0, 6.0, ((0, 4), (1, 32)))
    return dict(latents=latents, first_kernel=first_kernel, second_kernel=second_kernel, upstream=upstream)


def activate_grad(values):
    sigma = jax.nn.sigmoid(values)
    return sigma * (1.0 + values * (1.0 - sigma))

def flipped(kernel):
    return jnp.transpose(kernel[::-1, ::-1, ::-1], (0, 1, 2, 4, 3))

def gather_patches(padded, depth, offset, frames, height, across):
    channels = padded.shape[-1]
    window = padded[depth:depth + frames, offset:offset + height]
    parts = [window[:, :, lateral:lateral + across] for lateral in range(3)]
    return jnp.concatenate(parts, axis=-1).reshape(frames * height * across, 3 * channels)

def correlate(padded, kernel, frames, height, across):
    channels = padded.shape[-1]
    outward = kernel.shape[-1]
    summed = jnp.zeros((frames * height * across, outward), jnp.float32)
    for depth in range(3):
        for offset in range(3):
            patches = gather_patches(padded, depth, offset, frames, height, across)
            summed = summed + jnp.dot(patches, kernel[depth, offset].reshape(3 * channels, outward), preferred_element_type=jnp.float32)
    return summed.reshape(frames, height, across, outward)

def kernel_grad(padded, grad_rows, frames, height, across):
    channels = padded.shape[-1]
    outward = grad_rows.shape[-1]
    pieces = []
    for depth in range(3):
        for offset in range(3):
            patches = gather_patches(padded, depth, offset, frames, height, across)
            product = lax.dot_general(patches, grad_rows, (((0,), (0,)), ((), ())), preferred_element_type=jnp.float32)
            pieces.append(product.reshape(3, channels, outward))
    return jnp.stack(pieces).reshape(3, 3, 3, channels, outward)

def reference(latents, first_kernel, second_kernel, upstream):
    frames, height, across, channels = latents.shape
    before = ((2, 0), (1, 1), (1, 1), (0, 0))
    after = ((0, 2), (1, 1), (1, 1), (0, 0))
    inputs = latents.astype(jnp.float32)
    smooth = jax.nn.silu(inputs).astype(jnp.bfloat16)
    padded_in = jnp.pad(smooth, before)
    hidden = correlate(padded_in, first_kernel, frames, height, across)
    active = jax.nn.silu(hidden).astype(jnp.bfloat16)
    padded_mid = jnp.pad(active, before)
    branch = correlate(padded_mid, second_kernel, frames, height, across)
    decoded = (inputs + branch).astype(jnp.bfloat16)
    padded_up = jnp.pad(upstream, after)
    mid_grad = correlate(padded_up, flipped(second_kernel), frames, height, across)
    hidden_grad = (mid_grad * activate_grad(hidden)).astype(jnp.bfloat16)
    padded_hid = jnp.pad(hidden_grad, after)
    inner_grad = correlate(padded_hid, flipped(first_kernel), frames, height, across)
    latent_grad = (upstream.astype(jnp.float32) + inner_grad * activate_grad(inputs)).astype(jnp.bfloat16)
    second_grad = kernel_grad(padded_mid, upstream.reshape(-1, channels), frames, height, across)
    first_grad = kernel_grad(padded_in, hidden_grad.reshape(-1, channels), frames, height, across)
    return (decoded, latent_grad, first_grad, second_grad)
```

```python
import functools

import jax
import jax.numpy as jnp
from jax import lax
from jax.experimental import pallas as pl
from jax.experimental.pallas import tpu as pltpu
from jax.sharding import Mesh, PartitionSpec as P

GROUP = ("zl", "co")
SPACE = ("zh", "y", "x")
CHIPS = ("zl", "zh", "y", "x")
C = 256
W = 128
FRAMES = 4
EXT = FRAMES + 2
TAPS = 27
BF = jnp.bfloat16
F32 = jnp.float32
PASS_FLOPS = 2 * FRAMES * 2 * W * TAPS * C * C


def fill_ext(ext_ref, own_ref, rows_ref, time_ref, first, which):
    other = 0 if first == 2 else FRAMES
    for f in range(FRAMES):
        ext_ref[first + f, 0:W] = rows_ref[0, which, f]
        for r in range(2):
            ext_ref[first + f, (r + 1) * W : (r + 2) * W] = own_ref[f, r]
        ext_ref[first + f, 3 * W : 4 * W] = rows_ref[1, which, f]
    for f in range(2):
        for r in range(4):
            ext_ref[other + f, r * W : (r + 1) * W] = time_ref[f, r]


def shifted(value, by):
    height = value.shape[0]
    turned = pltpu.roll(value, by % height, 0)
    column = lax.broadcasted_iota(jnp.int32, value.shape, 0) % W
    edge = 0 if by > 0 else W - 1
    return jnp.where(column == edge, 0.0, turned)


def conv_frame(ext_ref, kernel_ref, t, transposed):
    parts = []
    for i in range(3):
        for j in range(3):
            frame = t + (2 - i if transposed else i)
            row = 2 - j if transposed else j
            parts.append(ext_ref[frame, row * W : (row + 2) * W])
    lhs = jnp.concatenate(parts, axis=1)
    sums = []
    for k in range(3):
        taps = [kernel_ref[(i * 3 + j) * 3 + k] for i in range(3) for j in range(3)]
        if transposed:
            rhs = jnp.concatenate(taps, axis=1)
            dims = (((1,), (1,)), ((), ()))
        else:
            rhs = jnp.concatenate(taps, axis=0)
            dims = (((1,), (0,)), ((), ()))
        sums.append(lax.dot_general(lhs, rhs, dims, preferred_element_type=F32))
    if transposed:
        return sums[1] + shifted(sums[0], -1) + shifted(sums[2], 1)
    return sums[1] + shifted(sums[0], 1) + shifted(sums[2], -1)


def gate_grad(values):
    s = jax.nn.sigmoid(values)
    return s * (1.0 + values * (1.0 - s))


def split_rows(value):
    return value.reshape(2, W, C)


def hidden_kernel(own_ref, rows_ref, time_ref, kernel_ref, hidden_ref, active_ref, ext_ref):
    fill_ext(ext_ref, own_ref, rows_ref, time_ref, 2, 0)

    def body(t, carry):
        hidden = conv_frame(ext_ref, kernel_ref, t, False)
        hidden_ref[t] = hidden
        active_ref[t] = split_rows((hidden * jax.nn.sigmoid(hidden)).astype(BF))
        return carry

    lax.fori_loop(0, FRAMES, body, 0)


def hidden_grad_kernel(own_ref, rows_ref, time_ref, kernel_ref, hidden_ref, out_ref, ext_ref):
    fill_ext(ext_ref, own_ref, rows_ref, time_ref, 0, 1)

    def body(t, carry):
        grad = conv_frame(ext_ref, kernel_ref, t, True)
        out_ref[t] = split_rows((grad * gate_grad(hidden_ref[t])).astype(BF))
        return carry

    lax.fori_loop(0, FRAMES, body, 0)


def decoded_kernel(own_ref, rows_ref, time_ref, kernel_ref, latents_ref, out_ref, ext_ref):
    fill_ext(ext_ref, own_ref, rows_ref, time_ref, 2, 0)

    def body(t, carry):
        branch = split_rows(conv_frame(ext_ref, kernel_ref, t, False))
        out_ref[t] = (latents_ref[t].astype(F32) + branch).astype(BF)
        return carry

    lax.fori_loop(0, FRAMES, body, 0)


def latent_grad_kernel(
    own_ref, rows_ref, time_ref, kernel_ref, latents_ref, upstream_ref, out_ref, ext_ref
):
    fill_ext(ext_ref, own_ref, rows_ref, time_ref, 0, 1)

    def body(t, carry):
        inner = split_rows(conv_frame(ext_ref, kernel_ref, t, True))
        gate = gate_grad(latents_ref[t].astype(F32))
        out_ref[t] = (upstream_ref[t].astype(F32) + inner * gate).astype(BF)
        return carry

    lax.fori_loop(0, FRAMES, body, 0)


def keep_first(core, value):
    return jnp.where(core == 0, value, pltpu.roll(value, C // 2, 0))


def shift_copies(value):
    wide = value.astype(F32)
    return [shifted(wide, -1).astype(BF), value, shifted(wide, 1).astype(BF)]


def put_tap(keep_ref, send_ref, tap, product):
    for ref, low in ((keep_ref, 0), (send_ref, C // 2)):
        half = product[low : low + C // 2].astype(ref.dtype)
        for b in range(2):
            ref[:, b, tap] = half[:, b * 128 : (b + 1) * 128].reshape(16, 8, 128)


def second_grad_kernel(
    core_ref, active_ref, own_ref, rows_ref, time_ref, keep_ref, send_ref, ext_ref, across_ref, turn_ref
):
    core = core_ref[0]
    fill_ext(ext_ref, own_ref, rows_ref, time_ref, 0, 1)
    for f in range(EXT):
        for k, copy in enumerate(shift_copies(ext_ref[f])):
            across_ref[k, f] = copy
    for t in range(FRAMES):
        flat = active_ref[t].reshape(2 * W, C).astype(F32)
        turn_ref[:, t * 2 * W : (t + 1) * 2 * W] = keep_first(core, flat.T).astype(BF)

    def body(i, carry):
        for j in range(3):
            for k in range(3):
                rhs = jnp.concatenate(
                    [across_ref[k, t + 2 - i, (2 - j) * W : (4 - j) * W] for t in range(FRAMES)], axis=0
                )
                product = jnp.dot(turn_ref[...], rhs, preferred_element_type=F32)
                put_tap(keep_ref, send_ref, i * 9 + j * 3 + k, product)
        return carry

    lax.fori_loop(0, 3, body, 0)


def first_grad_kernel(
    core_ref, grad_ref, own_ref, rows_ref, time_ref, keep_ref, send_ref, ext_ref, across_ref, turn_ref
):
    core = core_ref[0]
    fill_ext(ext_ref, own_ref, rows_ref, time_ref, 2, 0)
    for t in range(FRAMES):
        for k, copy in enumerate(shift_copies(grad_ref[t].reshape(2 * W, C))):
            across_ref[k, t * 2 * W : (t + 1) * 2 * W] = copy
    for f in range(EXT):
        turn_ref[f] = keep_first(core, ext_ref[f].astype(F32).T).astype(BF)

    def body(i, carry):
        for j in range(3):
            lhs = jnp.concatenate(
                [turn_ref[t + i, :, j * W : (j + 2) * W] for t in range(FRAMES)], axis=1
            )
            for k in range(3):
                product = jnp.dot(lhs, across_ref[k], preferred_element_type=F32)
                put_tap(keep_ref, send_ref, i * 9 + j * 3 + k, product)
        return carry

    lax.fori_loop(0, 3, body, 0)


def cost(flops, moved):
    return pl.CostEstimate(flops=flops, bytes_accessed=moved, transcendentals=0)


def whole(kernel, outs, scratch, limit, name, smem=0):
    def call(*args):
        moved = sum(a.size * a.dtype.itemsize for a in args)
        moved += sum(o.size * o.dtype.itemsize for o in outs)
        specs = [
            pl.BlockSpec(memory_space=pltpu.SMEM if n < smem else pltpu.VMEM) for n in range(len(args))
        ]
        return pl.pallas_call(
            kernel,
            out_shape=outs,
            in_specs=specs,
            out_specs=[pl.BlockSpec(memory_space=pltpu.VMEM) for _ in outs],
            scratch_shapes=scratch,
            compiler_params=pltpu.CompilerParams(vmem_limit_bytes=limit << 20),
            cost_estimate=cost(PASS_FLOPS, moved),
            name=name,
        )(*args)

    return call


STEP = 3


def assemble_kernel(core_ref, own2_ref, own1_ref, far2_ref, far1_ref, first_ref, second_ref):
    core = core_ref[0]
    mine = pl.multiple_of(core * 128, 128)
    theirs = pl.multiple_of((1 - core) * 128, 128)
    for out, own, far in ((second_ref, own2_ref, far2_ref), (first_ref, own1_ref, far1_ref)):
        for p in range(STEP):
            for b in range(2):
                lanes = slice(b * 128, (b + 1) * 128)
                out[p, pl.ds(mine, 128), lanes] = own[0, :, b, p].astype(F32).reshape(128, 128)
                out[p, pl.ds(theirs, 128), lanes] = far[0, :, b, p].astype(F32).reshape(128, 128)


def assemble(core, own, far):
    own, far = (v.reshape(2, 16, 2, TAPS, 8, 128) for v in (own, far))
    block = (1, 16, 2, STEP, 8, 128)
    second = pl.BlockSpec(block, lambda p: (0, 0, 0, p, 0, 0))
    first = pl.BlockSpec(block, lambda p: (1, 0, 0, p, 0, 0))
    out = pl.BlockSpec((STEP, C, C), lambda p: (p, 0, 0))
    shape = jax.ShapeDtypeStruct((TAPS, C, C), F32)
    return pl.pallas_call(
        assemble_kernel,
        out_shape=(shape, shape),
        grid=(TAPS // STEP,),
        in_specs=[pl.BlockSpec(memory_space=pltpu.SMEM), second, first, second, first],
        out_specs=(out, out),
        compiler_params=pltpu.CompilerParams(vmem_limit_bytes=16 << 20),
        cost_estimate=cost(1 << 24, 28 << 20),
        name="assemble",
    )(core, own, own, far, far)


def total_kernel(parts_ref, out_ref):
    count = parts_ref.shape[0]

    def body(p, carry):
        total = parts_ref[0, p].astype(F32)
        for n in range(1, count):
            total = total + parts_ref[n, p].astype(F32)
        rounded = total.astype(BF)
        for n in range(count):
            out_ref[n, p] = rounded
        return carry

    lax.fori_loop(0, parts_ref.shape[1], body, 0)


def swap(value, axis, steps):
    count = lax.axis_size(axis)
    pairs = [(n, n + steps) for n in range(count) if 0 <= n + steps < count]
    return lax.ppermute(value, axis, pairs)


def edge_rows(one, two):
    to_above = jnp.stack([one[:, 0], two[:, 0]])
    to_below = jnp.stack([one[:, 1], two[:, 1]])
    return jnp.stack([swap(to_below, SPACE, 1), swap(to_above, SPACE, -1)])


def two_frames(own, rows, which, start):
    frames = slice(start, start + 2)
    return jnp.concatenate(
        [rows[0, which, frames][:, None], own[frames], rows[1, which, frames][:, None]], axis=1
    )


def local(latents, first_kernel, second_kernel, upstream):
    core = lax.axis_index("co").astype(jnp.int32).reshape(1)
    k1 = first_kernel.reshape(TAPS, C, C)
    k2 = second_kernel.reshape(TAPS, C, C)
    wide = latents.astype(F32)
    smooth = (wide * jax.nn.sigmoid(wide)).astype(BF)
    block = jax.ShapeDtypeStruct((FRAMES, 2, W, C), BF)
    ext = pltpu.VMEM((EXT, 4 * W, C), BF)

    rows = edge_rows(smooth, upstream)
    smooth_time = swap(two_frames(smooth, rows, 0, 2), GROUP, 1)
    up_time = swap(two_frames(upstream, rows, 1, 0), GROUP, -1)
    hidden, active = whole(
        hidden_kernel, (jax.ShapeDtypeStruct((FRAMES, 2 * W, C), F32), block), [ext], 24, "hidden"
    )(smooth, rows, smooth_time, k1)
    (hidden_grad,) = whole(hidden_grad_kernel, (block,), [ext], 24, "hidden_grad")(
        upstream, rows, up_time, k2, hidden
    )

    late = edge_rows(active, hidden_grad)
    active_time = swap(two_frames(active, late, 0, 2), GROUP, 1)
    grad_time = swap(two_frames(hidden_grad, late, 1, 0), GROUP, -1)

    half = (16, 2, TAPS, 8, 128)
    pair = (jax.ShapeDtypeStruct(half, F32), jax.ShapeDtypeStruct(half, BF))
    keep2, send2 = whole(
        second_grad_kernel,
        pair,
        [ext, pltpu.VMEM((3, EXT, 4 * W, C), BF), pltpu.VMEM((C, FRAMES * 2 * W), BF)],
        40,
        "second_grad",
        1,
    )(core, active, upstream, rows, up_time)
    keep1, send1 = whole(
        first_grad_kernel,
        pair,
        [ext, pltpu.VMEM((3, FRAMES * 2 * W, C), BF), pltpu.VMEM((EXT, C, 4 * W), BF)],
        40,
        "first_grad",
        1,
    )(core, hidden_grad, smooth, rows, smooth_time)

    across = [(0, 1), (1, 0)]
    got2 = lax.ppermute(send2, "co", across)
    got1 = lax.ppermute(send1, "co", across)
    chips = lax.axis_size(CHIPS)
    mine = jnp.stack([(keep2 + got2.astype(F32)).astype(BF), (keep1 + got1.astype(F32)).astype(BF)])
    mine = mine.reshape(chips, 64 // chips * TAPS, 8, 128)
    parts = lax.all_to_all(mine, CHIPS, 0, 0, tiled=False)
    (spread,) = whole(total_kernel, (jax.ShapeDtypeStruct(parts.shape, BF),), [], 16, "total")(parts)
    own = lax.all_to_all(spread, CHIPS, 0, 0, tiled=False)
    far = lax.ppermute(own, "co", across)

    (decoded,) = whole(decoded_kernel, (block,), [ext], 24, "decoded")(
        active, late, active_time, k2, latents
    )
    (latent_grad,) = whole(latent_grad_kernel, (block,), [ext], 24, "latent_grad")(
        hidden_grad, late, grad_time, k1, latents, upstream
    )
    first_grad, second_grad = assemble(core, own, far)
    shape = first_kernel.shape
    return (decoded, latent_grad, first_grad.reshape(shape), second_grad.reshape(shape))


def solution(mesh, sizes=(2, 2, 2, 4, 4)):
    fine = Mesh(mesh.devices.reshape(sizes), ("zl", "co", "zh", "y", "x"))
    placed = (P(GROUP, SPACE, None, None), P(), P(), P(GROUP, SPACE, None, None))
    return jax.shard_map(
        local,
        mesh=fine,
        in_specs=placed,
        out_specs=(P(GROUP, SPACE, None, None), P(GROUP, SPACE, None, None), P(), P()),
        check_vma=False,
    )
```

```python
import jax
import jax.numpy as jnp
from jax import lax
from jax.experimental import pallas as pl
from jax.experimental.pallas import tpu as pltpu
from jax.sharding import Mesh, PartitionSpec as P


GROUP = ("zl", "co")
SPACE = ("zh", "y", "x")
CHIPS = ("zl", "zh", "y", "x")
C = 256
W = 128
FRAMES = 4
EXT = FRAMES + 2
TAPS = 27
SLOTS = 28
BF = jnp.bfloat16
F32 = jnp.float32
PASS_FLOPS = 2 * FRAMES * 2 * W * TAPS * C * C


def fill_ext(ext_ref, own_ref, above_ref, below_ref, time_ref, first):
    other = 0 if first == 2 else FRAMES
    for f in range(FRAMES):
        ext_ref[first + f, 0:W] = above_ref[f]
        for r in range(2):
            ext_ref[first + f, (r + 1) * W : (r + 2) * W] = own_ref[f, r]
        ext_ref[first + f, 3 * W : 4 * W] = below_ref[f]
    for f in range(2):
        for r in range(4):
            ext_ref[other + f, r * W : (r + 1) * W] = time_ref[f, r]


def shifted(value, by):
    height = value.shape[0]
    turned = pltpu.roll(value, by % height, 0)
    column = lax.broadcasted_iota(jnp.int32, value.shape, 0) % W
    edge = 0 if by > 0 else W - 1
    return jnp.where(column == edge, 0.0, turned)


def conv_frame(ext_ref, kernel_ref, t, transposed):
    parts = []
    for i in range(3):
        for j in range(3):
            frame = t + (2 - i if transposed else i)
            row = 2 - j if transposed else j
            parts.append(ext_ref[frame, row * W : (row + 2) * W])
    lhs = jnp.concatenate(parts, axis=1)
    sums = []
    for k in range(3):
        taps = [kernel_ref[(i * 3 + j) * 3 + k] for i in range(3) for j in range(3)]
        if transposed:
            rhs = jnp.concatenate(taps, axis=1)
            dims = (((1,), (1,)), ((), ()))
        else:
            rhs = jnp.concatenate(taps, axis=0)
            dims = (((1,), (0,)), ((), ()))
        sums.append(lax.dot_general(lhs, rhs, dims, preferred_element_type=F32))
    if transposed:
        return sums[1] + shifted(sums[0], -1) + shifted(sums[2], 1)
    return sums[1] + shifted(sums[0], 1) + shifted(sums[2], -1)


def gate_grad(values):
    s = jax.nn.sigmoid(values)
    return s * (1.0 + values * (1.0 - s))


def split_rows(value):
    return value.reshape(2, W, C)


def hidden_kernel(own_ref, above_ref, below_ref, time_ref, kernel_ref, hidden_ref, active_ref, ext_ref):
    fill_ext(ext_ref, own_ref, above_ref, below_ref, time_ref, 2)

    def body(t, carry):
        hidden = conv_frame(ext_ref, kernel_ref, t, False)
        hidden_ref[t] = hidden
        active_ref[t] = split_rows((hidden * jax.nn.sigmoid(hidden)).astype(BF))
        return carry

    lax.fori_loop(0, FRAMES, body, 0)


def hidden_grad_kernel(own_ref, above_ref, below_ref, time_ref, kernel_ref, hidden_ref, out_ref, ext_ref):
    fill_ext(ext_ref, own_ref, above_ref, below_ref, time_ref, 0)

    def body(t, carry):
        grad = conv_frame(ext_ref, kernel_ref, t, True)
        out_ref[t] = split_rows((grad * gate_grad(hidden_ref[t])).astype(BF))
        return carry

    lax.fori_loop(0, FRAMES, body, 0)


def decoded_kernel(own_ref, above_ref, below_ref, time_ref, kernel_ref, latents_ref, out_ref, ext_ref):
    fill_ext(ext_ref, own_ref, above_ref, below_ref, time_ref, 2)

    def body(t, carry):
        branch = split_rows(conv_frame(ext_ref, kernel_ref, t, False))
        out_ref[t] = (latents_ref[t].astype(F32) + branch).astype(BF)
        return carry

    lax.fori_loop(0, FRAMES, body, 0)


def latent_grad_kernel(
    own_ref, above_ref, below_ref, time_ref, kernel_ref, latents_ref, upstream_ref, out_ref, ext_ref
):
    fill_ext(ext_ref, own_ref, above_ref, below_ref, time_ref, 0)

    def body(t, carry):
        inner = split_rows(conv_frame(ext_ref, kernel_ref, t, True))
        gate = gate_grad(latents_ref[t].astype(F32))
        out_ref[t] = (upstream_ref[t].astype(F32) + inner * gate).astype(BF)
        return carry

    lax.fori_loop(0, FRAMES, body, 0)


def keep_first(core, value):
    return jnp.where(core == 0, value, pltpu.roll(value, C // 2, 0))


def shift_copies(value):
    wide = value.astype(F32)
    return [shifted(wide, -1).astype(BF), value, shifted(wide, 1).astype(BF)]


def put_tap(keep_ref, send_ref, tap, product):
    for ref, low in ((keep_ref, 0), (send_ref, C // 2)):
        half = product[low : low + C // 2].astype(ref.dtype)
        for b in range(2):
            ref[:, b, tap] = half[:, b * 128 : (b + 1) * 128].reshape(16, 8, 128)


def clear_slot(keep_ref, send_ref):
    for ref in (keep_ref, send_ref):
        ref[:, :, TAPS] = jnp.zeros((16, 2, 8, 128), ref.dtype)


def second_grad_kernel(
    core_ref, active_ref, own_ref, above_ref, below_ref, time_ref, keep_ref, send_ref, ext_ref, across_ref, turn_ref
):
    core = core_ref[0]
    fill_ext(ext_ref, own_ref, above_ref, below_ref, time_ref, 0)
    for f in range(EXT):
        for k, copy in enumerate(shift_copies(ext_ref[f])):
            across_ref[k, f] = copy
    for t in range(FRAMES):
        flat = active_ref[t].reshape(2 * W, C).astype(F32)
        turn_ref[:, t * 2 * W : (t + 1) * 2 * W] = keep_first(core, flat.T).astype(BF)

    def body(i, carry):
        for j in range(3):
            for k in range(3):
                rhs = jnp.concatenate(
                    [across_ref[k, t + 2 - i, (2 - j) * W : (4 - j) * W] for t in range(FRAMES)], axis=0
                )
                product = jnp.dot(turn_ref[...], rhs, preferred_element_type=F32)
                put_tap(keep_ref, send_ref, i * 9 + j * 3 + k, product)
        return carry

    lax.fori_loop(0, 3, body, 0)
    clear_slot(keep_ref, send_ref)


def first_grad_kernel(
    core_ref, grad_ref, own_ref, above_ref, below_ref, time_ref, keep_ref, send_ref, ext_ref, across_ref, turn_ref
):
    core = core_ref[0]
    fill_ext(ext_ref, own_ref, above_ref, below_ref, time_ref, 2)
    for t in range(FRAMES):
        for k, copy in enumerate(shift_copies(grad_ref[t].reshape(2 * W, C))):
            across_ref[k, t * 2 * W : (t + 1) * 2 * W] = copy
    for f in range(EXT):
        turn_ref[f] = keep_first(core, ext_ref[f].astype(F32).T).astype(BF)

    def body(i, carry):
        for j in range(3):
            lhs = jnp.concatenate(
                [turn_ref[t + i, :, j * W : (j + 2) * W] for t in range(FRAMES)], axis=1
            )
            for k in range(3):
                product = jnp.dot(lhs, across_ref[k], preferred_element_type=F32)
                put_tap(keep_ref, send_ref, i * 9 + j * 3 + k, product)
        return carry

    lax.fori_loop(0, 3, body, 0)
    clear_slot(keep_ref, send_ref)


def cost(flops, moved):
    return pl.CostEstimate(flops=flops, bytes_accessed=moved, transcendentals=0)


def whole(kernel, outs, scratch, limit, smem=0, flops=PASS_FLOPS):
    def call(*args):
        moved = sum(a.size * a.dtype.itemsize for a in args)
        moved += sum(o.size * o.dtype.itemsize for o in outs)
        specs = [
            pl.BlockSpec(memory_space=pltpu.SMEM if n < smem else pltpu.VMEM) for n in range(len(args))
        ]
        return pl.pallas_call(
            kernel,
            out_shape=outs,
            in_specs=specs,
            out_specs=[pl.BlockSpec(memory_space=pltpu.VMEM) for _ in outs],
            scratch_shapes=scratch,
            compiler_params=pltpu.CompilerParams(vmem_limit_bytes=limit << 20),
            cost_estimate=cost(flops, moved),
        )(*args)

    return call


def tie(value, *after):
    return lax.optimization_barrier((value, *after))[0]


STEP = 3


def assemble_kernel(core_ref, own_ref, far_ref, out_ref):
    core = core_ref[0]
    mine = pl.multiple_of(core * 128, 128)
    theirs = pl.multiple_of((1 - core) * 128, 128)
    for p in range(STEP):
        for b in range(2):
            lanes = slice(b * 128, (b + 1) * 128)
            out_ref[p, pl.ds(mine, 128), lanes] = own_ref[:, b, p].astype(F32).reshape(128, 128)
            out_ref[p, pl.ds(theirs, 128), lanes] = far_ref[:, b, p].astype(F32).reshape(128, 128)


def assemble(core, own, far):
    own, far = (v.reshape(HALF) for v in (own, far))
    part = pl.BlockSpec((16, 2, STEP, 8, 128), lambda p: (0, 0, p, 0, 0))
    return pl.pallas_call(
        assemble_kernel,
        out_shape=jax.ShapeDtypeStruct((TAPS, C, C), F32),
        grid=(TAPS // STEP,),
        in_specs=[pl.BlockSpec(memory_space=pltpu.SMEM), part, part],
        out_specs=pl.BlockSpec((STEP, C, C), lambda p: (p, 0, 0)),
        compiler_params=pltpu.CompilerParams(vmem_limit_bytes=16 << 20),
        cost_estimate=cost(1 << 24, 11 << 20),
        name="assemble",
    )(core, own, far)


def total_kernel(parts_ref, out_ref):
    count = parts_ref.shape[0]

    def body(p, carry):
        total = parts_ref[0, p].astype(F32)
        for n in range(1, count):
            total = total + parts_ref[n, p].astype(F32)
        rounded = total.astype(BF)
        for n in range(count):
            out_ref[n, p] = rounded
        return carry

    lax.fori_loop(0, parts_ref.shape[1], body, 0)


def add_kernel(keep_ref, got_ref, out_ref):
    for b in range(2):

        def body(p, carry):
            both = keep_ref[:, b, p] + got_ref[:, b, p].astype(F32)
            out_ref[:, b, p] = both.astype(BF)
            return carry

        lax.fori_loop(0, SLOTS, body, 0)


def swap(value, axis, steps):
    count = lax.axis_size(axis)
    pairs = [(n, n + steps) for n in range(count) if 0 <= n + steps < count]
    return lax.ppermute(value, axis, pairs)


def edge_rows(own):
    return (swap(own[:, 1], SPACE, 1), swap(own[:, 0], SPACE, -1))


def two_frames(own, rows, start):
    frames = slice(start, start + 2)
    above, below = rows
    return jnp.concatenate([above[frames][:, None], own[frames], below[frames][:, None]], axis=1)


HALF = (16, 2, SLOTS, 8, 128)
PAIR = (jax.ShapeDtypeStruct(HALF, F32), jax.ShapeDtypeStruct(HALF, BF))
ACROSS = [(0, 1), (1, 0)]


def add_pair(keep, got):
    shape = jax.ShapeDtypeStruct(HALF, BF)
    (mine,) = whole(add_kernel, (shape,), [], 16, flops=1 << 28)(keep, got)
    chips = lax.axis_size(CHIPS)
    return mine.reshape(chips, 64 // chips * 14, 8, 128)


def total(parts):
    (spread,) = whole(total_kernel, (jax.ShapeDtypeStruct(parts.shape, BF),), [], 16, flops=1 << 28)(parts)
    return spread


def exchange(value):
    return lax.all_to_all(value, CHIPS, 0, 0, tiled=False)


def step(latents, first_kernel, second_kernel, upstream):
    core = lax.axis_index("co").astype(jnp.int32).reshape(1)
    k1 = first_kernel.reshape(TAPS, C, C)
    k2 = second_kernel.reshape(TAPS, C, C)
    wide = latents.astype(F32)
    smooth = (wide * jax.nn.sigmoid(wide)).astype(BF)
    block = jax.ShapeDtypeStruct((FRAMES, 2, W, C), BF)
    ext = pltpu.VMEM((EXT, 4 * W, C), BF)

    rows = edge_rows(smooth)
    up_rows = edge_rows(upstream)
    smooth_time = swap(two_frames(smooth, rows, 2), GROUP, 1)
    up_time = swap(two_frames(upstream, up_rows, 0), GROUP, -1)
    hidden, active = whole(
        hidden_kernel, (jax.ShapeDtypeStruct((FRAMES, 2 * W, C), F32), block), [ext], 24
    )(smooth, *rows, smooth_time, k1)
    keep2, send2 = whole(
        second_grad_kernel, PAIR, [ext, pltpu.VMEM((3, EXT, 4 * W, C), BF), pltpu.VMEM((C, FRAMES * 2 * W), BF)], 40, 1
    )(core, active, upstream, *up_rows, up_time)
    (hidden_grad,) = whole(hidden_grad_kernel, (block,), [ext], 24)(upstream, *up_rows, up_time, k2, hidden)
    got2 = lax.ppermute(send2, "co", ACROSS)
    mine2 = add_pair(keep2, tie(got2, hidden_grad))
    parts2 = exchange(mine2)
    keep1, send1 = whole(
        first_grad_kernel, PAIR, [ext, pltpu.VMEM((3, FRAMES * 2 * W, C), BF), pltpu.VMEM((EXT, C, 4 * W), BF)], 40, 1
    )(core, tie(hidden_grad, mine2), smooth, *rows, smooth_time)
    got1 = lax.ppermute(send1, "co", ACROSS)

    active_rows = edge_rows(active)
    grad_rows = edge_rows(hidden_grad)
    active_time = swap(two_frames(active, active_rows, 2), GROUP, 1)
    grad_time = swap(two_frames(hidden_grad, grad_rows, 0), GROUP, -1)
    parts1 = exchange(add_pair(keep1, tie(got1, *grad_rows, active_time)))
    (decoded,) = whole(decoded_kernel, (block,), [ext], 24)(
        active, *active_rows, active_time, k2, latents
    )
    (latent_grad,) = whole(latent_grad_kernel, (block,), [ext], 24)(
        hidden_grad, *grad_rows, grad_time, k1, latents, upstream
    )
    own2 = exchange(total(tie(parts2, decoded)))
    own1 = exchange(total(tie(parts1, latent_grad)))
    far2 = lax.ppermute(own2, "co", ACROSS)
    far1 = lax.ppermute(own1, "co", ACROSS)
    second_grad = assemble(core, own2, far2)
    first_grad = assemble(core, own1, far1)
    shape = first_kernel.shape
    return (decoded, latent_grad, first_grad.reshape(shape), second_grad.reshape(shape))


def solution(mesh, sizes=(2, 2, 2, 4, 4)):
    fine = Mesh(mesh.devices.reshape(sizes), ("zl", "co", "zh", "y", "x"))
    placed = (P(GROUP, SPACE, None, None), P(), P(), P(GROUP, SPACE, None, None))
    return jax.shard_map(
        step,
        mesh=fine,
        in_specs=placed,
        out_specs=(P(GROUP, SPACE, None, None), P(GROUP, SPACE, None, None), P(), P()),
        check_vma=False,
    )
```

```python
import jax
import jax.numpy as jnp
from jax import lax
from jax.experimental import pallas as pl
from jax.experimental.pallas import tpu as pltpu
from jax.sharding import Mesh, PartitionSpec as P


GROUP = ("zl", "co")
SPACE = ("zh", "y", "x")
CHIPS = ("zl", "zh", "y", "x")
C = 256
W = 128
FRAMES = 4
EXT = FRAMES + 2
TAPS = 27
BF = jnp.bfloat16
F32 = jnp.float32
PASS_FLOPS = 2 * FRAMES * 2 * W * TAPS * C * C


def fill_ext(ext_ref, own_ref, rows_ref, time_ref, first, which):
    other = 0 if first == 2 else FRAMES
    for f in range(FRAMES):
        ext_ref[first + f, 0:W] = rows_ref[0, which, f]
        for r in range(2):
            ext_ref[first + f, (r + 1) * W : (r + 2) * W] = own_ref[f, r]
        ext_ref[first + f, 3 * W : 4 * W] = rows_ref[1, which, f]
    for f in range(2):
        for r in range(4):
            ext_ref[other + f, r * W : (r + 1) * W] = time_ref[f, r]


def shifted(value, by):
    height = value.shape[0]
    turned = pltpu.roll(value, by % height, 0)
    column = lax.broadcasted_iota(jnp.int32, value.shape, 0) % W
    edge = 0 if by > 0 else W - 1
    return jnp.where(column == edge, 0.0, turned)


def conv_frame(ext_ref, kernel_ref, t, transposed):
    parts = []
    for i in range(3):
        for j in range(3):
            frame = t + (2 - i if transposed else i)
            row = 2 - j if transposed else j
            parts.append(ext_ref[frame, row * W : (row + 2) * W])
    lhs = jnp.concatenate(parts, axis=1)
    sums = []
    for k in range(3):
        taps = [kernel_ref[k, n] for n in range(9)]
        if transposed:
            rhs = jnp.concatenate(taps, axis=1)
            dims = (((1,), (1,)), ((), ()))
        else:
            rhs = jnp.concatenate(taps, axis=0)
            dims = (((1,), (0,)), ((), ()))
        sums.append(lax.dot_general(lhs, rhs, dims, preferred_element_type=F32))
    if transposed:
        return sums[1] + shifted(sums[0], -1) + shifted(sums[2], 1)
    return sums[1] + shifted(sums[0], 1) + shifted(sums[2], -1)


def gate_grad(values):
    s = jax.nn.sigmoid(values)
    return s * (1.0 + values * (1.0 - s))


def load_taps(source_ref, kernel_ref, sem):
    copies = [
        pltpu.make_async_copy(source_ref.at[:, k], kernel_ref.at[k], sem.at[k]) for k in range(3)
    ]
    for copy in copies:
        copy.start()
    return copies


def split_rows(value):
    return value.reshape(2, W, C)


def hidden_kernel(own_ref, rows_ref, time_ref, source_ref, hidden_ref, active_ref, ext_ref, kernel_ref, sem):
    copies = load_taps(source_ref, kernel_ref, sem)
    fill_ext(ext_ref, own_ref, rows_ref, time_ref, 2, 0)
    for copy in copies:
        copy.wait()

    def body(t, carry):
        hidden = conv_frame(ext_ref, kernel_ref, t, False)
        hidden_ref[t] = hidden
        active_ref[t] = split_rows((hidden * jax.nn.sigmoid(hidden)).astype(BF))
        return carry

    lax.fori_loop(0, FRAMES, body, 0)


def hidden_grad_kernel(own_ref, rows_ref, time_ref, source_ref, hidden_ref, out_ref, ext_ref, kernel_ref, sem):
    copies = load_taps(source_ref, kernel_ref, sem)
    fill_ext(ext_ref, own_ref, rows_ref, time_ref, 0, 1)
    for copy in copies:
        copy.wait()

    def body(t, carry):
        grad = conv_frame(ext_ref, kernel_ref, t, True)
        out_ref[t] = split_rows((grad * gate_grad(hidden_ref[t])).astype(BF))
        return carry

    lax.fori_loop(0, FRAMES, body, 0)


def decoded_kernel(own_ref, rows_ref, time_ref, source_ref, latents_ref, out_ref, ext_ref, kernel_ref, sem):
    copies = load_taps(source_ref, kernel_ref, sem)
    fill_ext(ext_ref, own_ref, rows_ref, time_ref, 2, 0)
    for copy in copies:
        copy.wait()

    def body(t, carry):
        branch = split_rows(conv_frame(ext_ref, kernel_ref, t, False))
        out_ref[t] = (latents_ref[t].astype(F32) + branch).astype(BF)
        return carry

    lax.fori_loop(0, FRAMES, body, 0)


def latent_grad_kernel(
    own_ref, rows_ref, time_ref, source_ref, latents_ref, upstream_ref, out_ref, ext_ref, kernel_ref, sem
):
    copies = load_taps(source_ref, kernel_ref, sem)
    fill_ext(ext_ref, own_ref, rows_ref, time_ref, 0, 1)
    for copy in copies:
        copy.wait()

    def body(t, carry):
        inner = split_rows(conv_frame(ext_ref, kernel_ref, t, True))
        gate = gate_grad(latents_ref[t].astype(F32))
        out_ref[t] = (upstream_ref[t].astype(F32) + inner * gate).astype(BF)
        return carry

    lax.fori_loop(0, FRAMES, body, 0)


def keep_first(core, value):
    return jnp.where(core == 0, value, pltpu.roll(value, C // 2, 0))


def shift_copies(value):
    wide = value.astype(F32)
    return [shifted(wide, -1).astype(BF), value, shifted(wide, 1).astype(BF)]


def put_tap(keep_ref, send_ref, tap, product):
    for ref, low in ((keep_ref, 0), (send_ref, C // 2)):
        half = product[low : low + C // 2].astype(ref.dtype)
        for b in range(2):
            ref[:, b, tap] = half[:, b * 128 : (b + 1) * 128].reshape(16, 8, 128)


def second_grad_kernel(
    core_ref, active_ref, own_ref, rows_ref, time_ref, keep_ref, send_ref, ext_ref, across_ref, turn_ref
):
    core = core_ref[0]
    fill_ext(ext_ref, own_ref, rows_ref, time_ref, 0, 1)
    for f in range(EXT):
        for k, copy in enumerate(shift_copies(ext_ref[f])):
            across_ref[k, f] = copy
    for t in range(FRAMES):
        flat = active_ref[t].reshape(2 * W, C).astype(F32)
        turn_ref[:, t * 2 * W : (t + 1) * 2 * W] = keep_first(core, flat.T).astype(BF)

    def body(i, carry):
        for j in range(3):
            for k in range(3):
                rhs = jnp.concatenate(
                    [across_ref[k, t + 2 - i, (2 - j) * W : (4 - j) * W] for t in range(FRAMES)], axis=0
                )
                product = jnp.dot(turn_ref[...], rhs, preferred_element_type=F32)
                put_tap(keep_ref, send_ref, i * 9 + j * 3 + k, product)
        return carry

    lax.fori_loop(0, 3, body, 0)


def first_grad_kernel(
    core_ref, grad_ref, own_ref, rows_ref, time_ref, keep_ref, send_ref, ext_ref, across_ref, turn_ref
):
    core = core_ref[0]
    fill_ext(ext_ref, own_ref, rows_ref, time_ref, 2, 0)
    for t in range(FRAMES):
        for k, copy in enumerate(shift_copies(grad_ref[t].reshape(2 * W, C))):
            across_ref[k, t * 2 * W : (t + 1) * 2 * W] = copy
    for f in range(EXT):
        turn_ref[f] = keep_first(core, ext_ref[f].astype(F32).T).astype(BF)

    def body(i, carry):
        for j in range(3):
            lhs = jnp.concatenate(
                [turn_ref[t + i, :, j * W : (j + 2) * W] for t in range(FRAMES)], axis=1
            )
            for k in range(3):
                product = jnp.dot(lhs, across_ref[k], preferred_element_type=F32)
                put_tap(keep_ref, send_ref, i * 9 + j * 3 + k, product)
        return carry

    lax.fori_loop(0, 3, body, 0)


def cost(flops, moved):
    return pl.CostEstimate(flops=flops, bytes_accessed=moved, transcendentals=0)


def whole(kernel, outs, scratch, limit, smem=0, hbm=(), flops=PASS_FLOPS):
    def call(*args):
        moved = sum(a.size * a.dtype.itemsize for a in args)
        moved += sum(o.size * o.dtype.itemsize for o in outs)
        spaces = [
            pltpu.SMEM if n < smem else pltpu.HBM if n in hbm else pltpu.VMEM for n in range(len(args))
        ]
        return pl.pallas_call(
            kernel,
            out_shape=outs,
            in_specs=[pl.BlockSpec(memory_space=space) for space in spaces],
            out_specs=[pl.BlockSpec(memory_space=pltpu.VMEM) for _ in outs],
            scratch_shapes=scratch,
            compiler_params=pltpu.CompilerParams(vmem_limit_bytes=limit << 20),
            cost_estimate=cost(flops, moved),
        )(*args)

    return call


def convolution(kernel, outs):
    scratch = [
        pltpu.VMEM((EXT, 4 * W, C), BF),
        pltpu.VMEM((3, 9, C, C), BF),
        pltpu.SemaphoreType.DMA((3,)),
    ]
    return whole(kernel, outs, scratch, 24, hbm=(3,))


STEP = 3


def assemble_kernel(core_ref, own2_ref, own1_ref, far2_ref, far1_ref, first_ref, second_ref):
    core = core_ref[0]
    mine = pl.multiple_of(core * 128, 128)
    theirs = pl.multiple_of((1 - core) * 128, 128)
    for out, own, far in ((second_ref, own2_ref, far2_ref), (first_ref, own1_ref, far1_ref)):
        for p in range(STEP):
            for b in range(2):
                lanes = slice(b * 128, (b + 1) * 128)
                out[p, pl.ds(mine, 128), lanes] = own[0, :, b, p].astype(F32).reshape(128, 128)
                out[p, pl.ds(theirs, 128), lanes] = far[0, :, b, p].astype(F32).reshape(128, 128)


def assemble(core, own, far):
    own, far = (v.reshape(2, 16, 2, TAPS, 8, 128) for v in (own, far))
    block = (1, 16, 2, STEP, 8, 128)
    second = pl.BlockSpec(block, lambda p: (0, 0, 0, p, 0, 0))
    first = pl.BlockSpec(block, lambda p: (1, 0, 0, p, 0, 0))
    out = pl.BlockSpec((STEP, C, C), lambda p: (p, 0, 0))
    shape = jax.ShapeDtypeStruct((TAPS, C, C), F32)
    return pl.pallas_call(
        assemble_kernel,
        out_shape=(shape, shape),
        grid=(TAPS // STEP,),
        in_specs=[pl.BlockSpec(memory_space=pltpu.SMEM), second, first, second, first],
        out_specs=(out, out),
        compiler_params=pltpu.CompilerParams(vmem_limit_bytes=16 << 20),
        cost_estimate=cost(1 << 24, 28 << 20),
        name="assemble",
    )(core, own, own, far, far)


def total_kernel(parts_ref, out_ref):
    count = parts_ref.shape[0]

    def body(p, carry):
        total = parts_ref[0, p].astype(F32)
        for n in range(1, count):
            total = total + parts_ref[n, p].astype(F32)
        rounded = total.astype(BF)
        for n in range(count):
            out_ref[n, p] = rounded
        return carry

    lax.fori_loop(0, parts_ref.shape[1], body, 0)


def swap(value, axis, steps):
    count = lax.axis_size(axis)
    pairs = [(n, n + steps) for n in range(count) if 0 <= n + steps < count]
    return lax.ppermute(value, axis, pairs)


def edge_rows(one, two):
    to_above = jnp.stack([one[:, 0], two[:, 0]])
    to_below = jnp.stack([one[:, 1], two[:, 1]])
    above = swap(to_below, SPACE, 1)
    below = swap(to_above, SPACE, -1)
    return jnp.stack([above, below])


def two_frames(own, rows, which, start):
    frames = slice(start, start + 2)
    return jnp.concatenate(
        [rows[0, which, frames][:, None], own[frames], rows[1, which, frames][:, None]], axis=1
    )


def step(latents, first_kernel, second_kernel, upstream):
    core = lax.axis_index("co").astype(jnp.int32).reshape(1)
    k1 = first_kernel.reshape(9, 3, C, C)
    k2 = second_kernel.reshape(9, 3, C, C)
    wide = latents.astype(F32)
    smooth = (wide * jax.nn.sigmoid(wide)).astype(BF)
    block = jax.ShapeDtypeStruct((FRAMES, 2, W, C), BF)
    ext = pltpu.VMEM((EXT, 4 * W, C), BF)

    rows = edge_rows(smooth, upstream)
    smooth_time = swap(two_frames(smooth, rows, 0, 2), GROUP, 1)
    up_time = swap(two_frames(upstream, rows, 1, 0), GROUP, -1)
    hidden, active = convolution(
        hidden_kernel, (jax.ShapeDtypeStruct((FRAMES, 2 * W, C), F32), block)
    )(smooth, rows, smooth_time, k1)
    (hidden_grad,) = convolution(hidden_grad_kernel, (block,))(
        upstream, rows, up_time, k2, hidden
    )

    late = edge_rows(active, hidden_grad)
    active_time = swap(two_frames(active, late, 0, 2), GROUP, 1)
    grad_time = swap(two_frames(hidden_grad, late, 1, 0), GROUP, -1)

    half = (16, 2, TAPS, 8, 128)
    pair = (jax.ShapeDtypeStruct(half, F32), jax.ShapeDtypeStruct(half, BF))
    keep2, send2 = whole(
        second_grad_kernel, pair, [ext, pltpu.VMEM((3, EXT, 4 * W, C), BF), pltpu.VMEM((C, FRAMES * 2 * W), BF)], 40, 1
    )(core, active, upstream, rows, up_time)
    keep1, send1 = whole(
        first_grad_kernel, pair, [ext, pltpu.VMEM((3, FRAMES * 2 * W, C), BF), pltpu.VMEM((EXT, C, 4 * W), BF)], 40, 1
    )(core, hidden_grad, smooth, rows, smooth_time)

    across = [(0, 1), (1, 0)]
    got2 = lax.ppermute(send2, "co", across)
    got1 = lax.ppermute(send1, "co", across)
    chips = lax.axis_size(CHIPS)
    mine = jnp.stack([(keep2 + got2.astype(F32)).astype(BF), (keep1 + got1.astype(F32)).astype(BF)])
    mine = mine.reshape(chips, 64 // chips * TAPS, 8, 128)
    parts = lax.all_to_all(mine, CHIPS, 0, 0, tiled=False)
    (spread,) = whole(total_kernel, (jax.ShapeDtypeStruct(parts.shape, BF),), [], 16, flops=1 << 28)(parts)
    own = lax.all_to_all(spread, CHIPS, 0, 0, tiled=False)
    far = lax.ppermute(own, "co", across)

    (decoded,) = convolution(decoded_kernel, (block,))(
        active, late, active_time, k2, latents
    )
    (latent_grad,) = convolution(latent_grad_kernel, (block,))(hidden_grad, late, grad_time, k1, latents, upstream)
    first_grad, second_grad = assemble(core, own, far)
    shape = first_kernel.shape
    return (decoded, latent_grad, first_grad.reshape(shape), second_grad.reshape(shape))


def solution(mesh, sizes=(2, 2, 2, 4, 4)):
    fine = Mesh(mesh.devices.reshape(sizes), ("zl", "co", "zh", "y", "x"))
    placed = (P(GROUP, SPACE, None, None), P(), P(), P(GROUP, SPACE, None, None))
    return jax.shard_map(
        step,
        mesh=fine,
        in_specs=placed,
        out_specs=(P(GROUP, SPACE, None, None), P(GROUP, SPACE, None, None), P(), P()),
        check_vma=False,
    )
```

```python
import math

import jax
import jax.numpy as jnp
import numpy as np
from jax import lax
from jax.experimental import pallas as pl
from jax.experimental.pallas import tpu as pltpu
from jax.sharding import Mesh, PartitionSpec as P


GROUP = ("zl", "co")
SPACE = ("zh", "y", "x")
ALL = ("zl", "co", "zh", "y", "x")
C = 256
W = 128
FRAMES = 4
EXT = FRAMES + 2
TAPS = 27
BF = jnp.bfloat16
F32 = jnp.float32
PASS_FLOPS = 2 * FRAMES * 2 * W * TAPS * C * C


def fill_ext(ext_ref, own_ref, rows_ref, time_ref, first, which):
    other = 0 if first == 2 else FRAMES
    for f in range(FRAMES):
        ext_ref[first + f, 0:W] = rows_ref[0, which, f]
        for r in range(2):
            ext_ref[first + f, (r + 1) * W : (r + 2) * W] = own_ref[f, r]
        ext_ref[first + f, 3 * W : 4 * W] = rows_ref[1, which, f]
    for f in range(2):
        for r in range(4):
            ext_ref[other + f, r * W : (r + 1) * W] = time_ref[f, r]


def shifted(value, by):
    height = value.shape[0]
    turned = pltpu.roll(value, by % height, 0)
    column = lax.broadcasted_iota(jnp.int32, value.shape, 0) % W
    edge = 0 if by > 0 else W - 1
    return jnp.where(column == edge, 0.0, turned)


def conv_frame(ext_ref, kernel_ref, t, transposed):
    parts = []
    for i in range(3):
        for j in range(3):
            frame = t + (2 - i if transposed else i)
            row = 2 - j if transposed else j
            parts.append(ext_ref[frame, row * W : (row + 2) * W])
    lhs = jnp.concatenate(parts, axis=1)
    sums = []
    for k in range(3):
        taps = [kernel_ref[k, n] for n in range(9)]
        if transposed:
            rhs = jnp.concatenate(taps, axis=1)
            dims = (((1,), (1,)), ((), ()))
        else:
            rhs = jnp.concatenate(taps, axis=0)
            dims = (((1,), (0,)), ((), ()))
        sums.append(lax.dot_general(lhs, rhs, dims, preferred_element_type=F32))
    if transposed:
        return sums[1] + shifted(sums[0], -1) + shifted(sums[2], 1)
    return sums[1] + shifted(sums[0], 1) + shifted(sums[2], -1)


def gate_grad(values):
    s = jax.nn.sigmoid(values)
    return s * (1.0 + values * (1.0 - s))


def load_taps(source_ref, kernel_ref, sem):
    copies = [
        pltpu.make_async_copy(source_ref.at[:, k], kernel_ref.at[k], sem.at[k]) for k in range(3)
    ]
    for copy in copies:
        copy.start()
    return copies


def split_rows(value):
    return value.reshape(2, W, C)


def hidden_kernel(own_ref, rows_ref, time_ref, source_ref, hidden_ref, active_ref, ext_ref, kernel_ref, sem):
    copies = load_taps(source_ref, kernel_ref, sem)
    fill_ext(ext_ref, own_ref, rows_ref, time_ref, 2, 0)
    for copy in copies:
        copy.wait()

    def body(t, carry):
        hidden = conv_frame(ext_ref, kernel_ref, t, False)
        hidden_ref[t] = hidden
        active_ref[t] = split_rows((hidden * jax.nn.sigmoid(hidden)).astype(BF))
        return carry

    lax.fori_loop(0, FRAMES, body, 0)


def hidden_grad_kernel(own_ref, rows_ref, time_ref, source_ref, hidden_ref, out_ref, ext_ref, kernel_ref, sem):
    copies = load_taps(source_ref, kernel_ref, sem)
    fill_ext(ext_ref, own_ref, rows_ref, time_ref, 0, 1)
    for copy in copies:
        copy.wait()

    def body(t, carry):
        grad = conv_frame(ext_ref, kernel_ref, t, True)
        out_ref[t] = split_rows((grad * gate_grad(hidden_ref[t])).astype(BF))
        return carry

    lax.fori_loop(0, FRAMES, body, 0)


def decoded_kernel(own_ref, rows_ref, time_ref, source_ref, latents_ref, out_ref, ext_ref, kernel_ref, sem):
    copies = load_taps(source_ref, kernel_ref, sem)
    fill_ext(ext_ref, own_ref, rows_ref, time_ref, 2, 0)
    for copy in copies:
        copy.wait()

    def body(t, carry):
        branch = split_rows(conv_frame(ext_ref, kernel_ref, t, False))
        out_ref[t] = (latents_ref[t].astype(F32) + branch).astype(BF)
        return carry

    lax.fori_loop(0, FRAMES, body, 0)


def latent_grad_kernel(
    own_ref, rows_ref, time_ref, source_ref, latents_ref, upstream_ref, out_ref, ext_ref, kernel_ref, sem
):
    copies = load_taps(source_ref, kernel_ref, sem)
    fill_ext(ext_ref, own_ref, rows_ref, time_ref, 0, 1)
    for copy in copies:
        copy.wait()

    def body(t, carry):
        inner = split_rows(conv_frame(ext_ref, kernel_ref, t, True))
        gate = gate_grad(latents_ref[t].astype(F32))
        out_ref[t] = (upstream_ref[t].astype(F32) + inner * gate).astype(BF)
        return carry

    lax.fori_loop(0, FRAMES, body, 0)


def keep_first(core, value):
    return jnp.where(core == 0, value, pltpu.roll(value, C // 2, 0))


def shift_copies(value):
    wide = value.astype(F32)
    return [shifted(wide, -1).astype(BF), value, shifted(wide, 1).astype(BF)]


def put_tap(keep_ref, send_ref, tap, product):
    for ref, low in ((keep_ref, 0), (send_ref, C // 2)):
        half = product[low : low + C // 2].astype(ref.dtype)
        for b in range(2):
            ref[:, b, tap] = half[:, b * 128 : (b + 1) * 128].reshape(16, 8, 128)


def second_grad_kernel(
    core_ref, active_ref, own_ref, rows_ref, time_ref, keep_ref, send_ref, ext_ref, across_ref, turn_ref
):
    core = core_ref[0]
    fill_ext(ext_ref, own_ref, rows_ref, time_ref, 0, 1)
    for f in range(EXT):
        for k, copy in enumerate(shift_copies(ext_ref[f])):
            across_ref[k, f] = copy
    for t in range(FRAMES):
        flat = active_ref[t].reshape(2 * W, C).astype(F32)
        turn_ref[:, t * 2 * W : (t + 1) * 2 * W] = keep_first(core, flat.T).astype(BF)

    def body(i, carry):
        for j in range(3):
            for k in range(3):
                rhs = jnp.concatenate(
                    [across_ref[k, t + 2 - i, (2 - j) * W : (4 - j) * W] for t in range(FRAMES)], axis=0
                )
                product = jnp.dot(turn_ref[...], rhs, preferred_element_type=F32)
                put_tap(keep_ref, send_ref, i * 9 + j * 3 + k, product)
        return carry

    lax.fori_loop(0, 3, body, 0)


def first_grad_kernel(
    core_ref, grad_ref, own_ref, rows_ref, time_ref, keep_ref, send_ref, ext_ref, across_ref, turn_ref
):
    core = core_ref[0]
    fill_ext(ext_ref, own_ref, rows_ref, time_ref, 2, 0)
    for t in range(FRAMES):
        for k, copy in enumerate(shift_copies(grad_ref[t].reshape(2 * W, C))):
            across_ref[k, t * 2 * W : (t + 1) * 2 * W] = copy
    for f in range(EXT):
        turn_ref[f] = keep_first(core, ext_ref[f].astype(F32).T).astype(BF)

    def body(i, carry):
        for j in range(3):
            lhs = jnp.concatenate(
                [turn_ref[t + i, :, j * W : (j + 2) * W] for t in range(FRAMES)], axis=1
            )
            for k in range(3):
                product = jnp.dot(lhs, across_ref[k], preferred_element_type=F32)
                put_tap(keep_ref, send_ref, i * 9 + j * 3 + k, product)
        return carry

    lax.fori_loop(0, 3, body, 0)


def cost(flops, moved):
    return pl.CostEstimate(flops=flops, bytes_accessed=moved, transcendentals=0)


def whole(kernel, outs, scratch, limit, smem=0, hbm=(), flops=PASS_FLOPS):
    def call(*args):
        moved = sum(a.size * a.dtype.itemsize for a in args)
        moved += sum(o.size * o.dtype.itemsize for o in outs)
        spaces = [
            pltpu.SMEM if n < smem else pltpu.HBM if n in hbm else pltpu.VMEM for n in range(len(args))
        ]
        return pl.pallas_call(
            kernel,
            out_shape=outs,
            in_specs=[pl.BlockSpec(memory_space=space) for space in spaces],
            out_specs=[pl.BlockSpec(memory_space=pltpu.VMEM) for _ in outs],
            scratch_shapes=scratch,
            compiler_params=pltpu.CompilerParams(vmem_limit_bytes=limit << 20),
            cost_estimate=cost(flops, moved),
        )(*args)

    return call


def convolution(kernel, outs):
    scratch = [
        pltpu.VMEM((EXT, 4 * W, C), BF),
        pltpu.VMEM((3, 9, C, C), BF),
        pltpu.SemaphoreType.DMA((3,)),
    ]
    return whole(kernel, outs, scratch, 24, hbm=(3,))


STEP = 3


def assemble_kernel(core_ref, own2_ref, own1_ref, far2_ref, far1_ref, first_ref, second_ref):
    core = core_ref[0]
    mine = pl.multiple_of(core * 128, 128)
    theirs = pl.multiple_of((1 - core) * 128, 128)
    for out, own, far in ((second_ref, own2_ref, far2_ref), (first_ref, own1_ref, far1_ref)):
        for p in range(STEP):
            for b in range(2):
                lanes = slice(b * 128, (b + 1) * 128)
                out[p, pl.ds(mine, 128), lanes] = own[0, :, b, p].astype(F32).reshape(128, 128)
                out[p, pl.ds(theirs, 128), lanes] = far[0, :, b, p].astype(F32).reshape(128, 128)


def assemble(core, own, far):
    own, far = (v.reshape(2, 16, 2, TAPS, 8, 128) for v in (own, far))
    block = (1, 16, 2, STEP, 8, 128)
    second = pl.BlockSpec(block, lambda p: (0, 0, 0, p, 0, 0))
    first = pl.BlockSpec(block, lambda p: (1, 0, 0, p, 0, 0))
    out = pl.BlockSpec((STEP, C, C), lambda p: (p, 0, 0))
    shape = jax.ShapeDtypeStruct((TAPS, C, C), F32)
    return pl.pallas_call(
        assemble_kernel,
        out_shape=(shape, shape),
        grid=(TAPS // STEP,),
        in_specs=[pl.BlockSpec(memory_space=pltpu.SMEM), second, first, second, first],
        out_specs=(out, out),
        compiler_params=pltpu.CompilerParams(vmem_limit_bytes=16 << 20),
        cost_estimate=cost(1 << 24, 28 << 20),
        name="assemble",
    )(core, own, own, far, far)


def total_kernel(parts_ref, out_ref):
    def body(q, carry):
        value = parts_ref[0, q].astype(F32)
        for n in range(1, parts_ref.shape[0]):
            value = value + parts_ref[n, q].astype(F32)
        rounded = value.astype(BF)
        for n in range(out_ref.shape[0]):
            out_ref[n, q] = rounded
        return carry

    lax.fori_loop(0, parts_ref.shape[1], body, 0)


def total(parts, copies):
    shape = jax.ShapeDtypeStruct((copies, *parts.shape[1:]), BF)
    return whole(total_kernel, (shape,), [], 16, flops=1 << 28)(parts)[0]


def stage_groups():
    sizes = [lax.axis_size(axis) for axis in ALL]
    grid = np.arange(math.prod(sizes)).reshape(sizes)
    near, rest = ([], [])
    for core, axis in ((0, 3), (1, 2)):
        chips = np.moveaxis(grid[:, core], axis, -1)
        lines = chips.reshape(-1, chips.shape[-1])
        near += lines.tolist()
        rest += lines.T.tolist()
    return near, rest


def exchange(value, groups):
    return lax.all_to_all(value, ALL, 0, 0, axis_index_groups=groups, tiled=False)


def swap(value, axis, steps):
    count = lax.axis_size(axis)
    pairs = [(n, n + steps) for n in range(count) if 0 <= n + steps < count]
    return lax.ppermute(value, axis, pairs)


def edge_rows(one, two):
    to_above = jnp.stack([one[:, 0], two[:, 0]])
    to_below = jnp.stack([one[:, 1], two[:, 1]])
    above = swap(to_below, SPACE, 1)
    below = swap(to_above, SPACE, -1)
    return jnp.stack([above, below])


def two_frames(own, rows, which, start):
    frames = slice(start, start + 2)
    return jnp.concatenate(
        [rows[0, which, frames][:, None], own[frames], rows[1, which, frames][:, None]], axis=1
    )


def step(latents, first_kernel, second_kernel, upstream):
    core = lax.axis_index("co").astype(jnp.int32).reshape(1)
    k1 = first_kernel.reshape(9, 3, C, C)
    k2 = second_kernel.reshape(9, 3, C, C)
    wide = latents.astype(F32)
    smooth = (wide * jax.nn.sigmoid(wide)).astype(BF)
    block = jax.ShapeDtypeStruct((FRAMES, 2, W, C), BF)
    ext = pltpu.VMEM((EXT, 4 * W, C), BF)

    rows = edge_rows(smooth, upstream)
    smooth_time = swap(two_frames(smooth, rows, 0, 2), GROUP, 1)
    up_time = swap(two_frames(upstream, rows, 1, 0), GROUP, -1)
    hidden, active = convolution(
        hidden_kernel, (jax.ShapeDtypeStruct((FRAMES, 2 * W, C), F32), block)
    )(smooth, rows, smooth_time, k1)
    (hidden_grad,) = convolution(hidden_grad_kernel, (block,))(
        upstream, rows, up_time, k2, hidden
    )

    late = edge_rows(active, hidden_grad)
    active_time = swap(two_frames(active, late, 0, 2), GROUP, 1)
    grad_time = swap(two_frames(hidden_grad, late, 1, 0), GROUP, -1)

    half = (16, 2, TAPS, 8, 128)
    pair = (jax.ShapeDtypeStruct(half, F32), jax.ShapeDtypeStruct(half, BF))
    keep2, send2 = whole(
        second_grad_kernel, pair, [ext, pltpu.VMEM((3, EXT, 4 * W, C), BF), pltpu.VMEM((C, FRAMES * 2 * W), BF)], 40, 1
    )(core, active, upstream, rows, up_time)
    keep1, send1 = whole(
        first_grad_kernel, pair, [ext, pltpu.VMEM((3, FRAMES * 2 * W, C), BF), pltpu.VMEM((EXT, C, 4 * W), BF)], 40, 1
    )(core, hidden_grad, smooth, rows, smooth_time)

    across = [(0, 1), (1, 0)]
    got2 = lax.ppermute(send2, "co", across)
    got1 = lax.ppermute(send1, "co", across)
    mine = jnp.stack([(keep2 + got2.astype(F32)).astype(BF), (keep1 + got1.astype(F32)).astype(BF)])
    near, rest = stage_groups()
    first, second = (len(near[0]), len(rest[0]))
    block_rows = 64 // (first * second) * TAPS
    parts = exchange(mine.reshape(first, second, block_rows, 8, 128), near)
    quarter = total(parts, 1)
    parts = exchange(quarter.reshape(second, block_rows, 8, 128), rest)
    spread = total(parts[:, None], second)
    quarter = exchange(spread.reshape(second, block_rows, 8, 128), rest)
    own = exchange(jnp.broadcast_to(quarter[None], (first, *quarter.shape)), near)
    far = lax.ppermute(own, "co", across)

    (decoded,) = convolution(decoded_kernel, (block,))(
        active, late, active_time, k2, latents
    )
    (latent_grad,) = convolution(latent_grad_kernel, (block,))(hidden_grad, late, grad_time, k1, latents, upstream)
    first_grad, second_grad = assemble(core, own, far)
    shape = first_kernel.shape
    return (decoded, latent_grad, first_grad.reshape(shape), second_grad.reshape(shape))


def solution(mesh, sizes=(2, 2, 2, 4, 4)):
    fine = Mesh(mesh.devices.reshape(sizes), ("zl", "co", "zh", "y", "x"))
    placed = (P(GROUP, SPACE, None, None), P(), P(), P(GROUP, SPACE, None, None))
    return jax.shard_map(
        step,
        mesh=fine,
        in_specs=placed,
        out_specs=(P(GROUP, SPACE, None, None), P(GROUP, SPACE, None, None), P(), P()),
        check_vma=False,
    )
```

```python
import math

import jax
import jax.numpy as jnp
import numpy as np
from jax import lax
from jax.experimental import pallas as pl
from jax.experimental.pallas import tpu as pltpu
from jax.sharding import Mesh, PartitionSpec as P


GROUP = ("zl", "co")
SPACE = ("zh", "y", "x")
ALL = ("zl", "co", "zh", "y", "x")
C = 256
W = 128
FRAMES = 4
EXT = FRAMES + 2
TAPS = 27
BF = jnp.bfloat16
F32 = jnp.float32
PASS_FLOPS = 2 * FRAMES * 2 * W * TAPS * C * C


def fill_ext(ext_ref, own_ref, rows_ref, time_ref, first, which):
    other = 0 if first == 2 else FRAMES
    for f in range(FRAMES):
        ext_ref[first + f, 0:W] = rows_ref[0, which, f]
        for r in range(2):
            ext_ref[first + f, (r + 1) * W : (r + 2) * W] = own_ref[f, r]
        ext_ref[first + f, 3 * W : 4 * W] = rows_ref[1, which, f]
    for f in range(2):
        for r in range(4):
            ext_ref[other + f, r * W : (r + 1) * W] = time_ref[f, r]


def shifted(value, by):
    height = value.shape[0]
    turned = pltpu.roll(value, by % height, 0)
    column = lax.broadcasted_iota(jnp.int32, value.shape, 0) % W
    edge = 0 if by > 0 else W - 1
    return jnp.where(column == edge, 0.0, turned)


def conv_frame(ext_ref, kernel_ref, t, transposed):
    parts = []
    for i in range(3):
        for j in range(3):
            frame = t + (2 - i if transposed else i)
            row = 2 - j if transposed else j
            parts.append(ext_ref[frame, row * W : (row + 2) * W])
    lhs = jnp.concatenate(parts, axis=1)
    sums = []
    for k in range(3):
        taps = [kernel_ref[k, n] for n in range(9)]
        if transposed:
            rhs = jnp.concatenate(taps, axis=1)
            dims = (((1,), (1,)), ((), ()))
        else:
            rhs = jnp.concatenate(taps, axis=0)
            dims = (((1,), (0,)), ((), ()))
        sums.append(lax.dot_general(lhs, rhs, dims, preferred_element_type=F32))
    if transposed:
        return sums[1] + shifted(sums[0], -1) + shifted(sums[2], 1)
    return sums[1] + shifted(sums[0], 1) + shifted(sums[2], -1)


def gate_grad(values):
    s = jax.nn.sigmoid(values)
    return s * (1.0 + values * (1.0 - s))


def load_taps(source_ref, kernel_ref, sem):
    copies = [
        pltpu.make_async_copy(source_ref.at[:, k], kernel_ref.at[k], sem.at[k]) for k in range(3)
    ]
    for copy in copies:
        copy.start()
    return copies


def split_rows(value):
    return value.reshape(2, W, C)


def hidden_kernel(own_ref, rows_ref, time_ref, source_ref, hidden_ref, active_ref, ext_ref, kernel_ref, sem):
    copies = load_taps(source_ref, kernel_ref, sem)
    fill_ext(ext_ref, own_ref, rows_ref, time_ref, 2, 0)
    for copy in copies:
        copy.wait()

    def body(t, carry):
        hidden = conv_frame(ext_ref, kernel_ref, t, False)
        hidden_ref[t] = hidden
        active_ref[t] = split_rows((hidden * jax.nn.sigmoid(hidden)).astype(BF))
        return carry

    lax.fori_loop(0, FRAMES, body, 0)


def hidden_grad_kernel(own_ref, rows_ref, time_ref, source_ref, hidden_ref, out_ref, ext_ref, kernel_ref, sem):
    copies = load_taps(source_ref, kernel_ref, sem)
    fill_ext(ext_ref, own_ref, rows_ref, time_ref, 0, 1)
    for copy in copies:
        copy.wait()

    def body(t, carry):
        grad = conv_frame(ext_ref, kernel_ref, t, True)
        out_ref[t] = split_rows((grad * gate_grad(hidden_ref[t])).astype(BF))
        return carry

    lax.fori_loop(0, FRAMES, body, 0)


def decoded_kernel(own_ref, rows_ref, time_ref, source_ref, latents_ref, out_ref, ext_ref, kernel_ref, sem):
    copies = load_taps(source_ref, kernel_ref, sem)
    fill_ext(ext_ref, own_ref, rows_ref, time_ref, 2, 0)
    for copy in copies:
        copy.wait()

    def body(t, carry):
        branch = split_rows(conv_frame(ext_ref, kernel_ref, t, False))
        out_ref[t] = (latents_ref[t].astype(F32) + branch).astype(BF)
        return carry

    lax.fori_loop(0, FRAMES, body, 0)


def latent_grad_kernel(
    own_ref, rows_ref, time_ref, source_ref, latents_ref, upstream_ref, out_ref, ext_ref, kernel_ref, sem
):
    copies = load_taps(source_ref, kernel_ref, sem)
    fill_ext(ext_ref, own_ref, rows_ref, time_ref, 0, 1)
    for copy in copies:
        copy.wait()

    def body(t, carry):
        inner = split_rows(conv_frame(ext_ref, kernel_ref, t, True))
        gate = gate_grad(latents_ref[t].astype(F32))
        out_ref[t] = (upstream_ref[t].astype(F32) + inner * gate).astype(BF)
        return carry

    lax.fori_loop(0, FRAMES, body, 0)


def keep_first(core, value):
    return jnp.where(core == 0, value, pltpu.roll(value, C // 2, 0))


def shift_copies(value):
    wide = value.astype(F32)
    return [shifted(wide, -1).astype(BF), value, shifted(wide, 1).astype(BF)]


def put_tap(keep_ref, send_ref, tap, product):
    for ref, low in ((keep_ref, 0), (send_ref, C // 2)):
        half = product[low : low + C // 2].astype(ref.dtype)
        for b in range(2):
            ref[:, b, tap] = half[:, b * 128 : (b + 1) * 128].reshape(16, 8, 128)


def second_grad_kernel(
    core_ref, active_ref, own_ref, rows_ref, time_ref, keep_ref, send_ref, ext_ref, across_ref, turn_ref
):
    core = core_ref[0]
    fill_ext(ext_ref, own_ref, rows_ref, time_ref, 0, 1)
    for f in range(EXT):
        for k, copy in enumerate(shift_copies(ext_ref[f])):
            across_ref[k, f] = copy
    for t in range(FRAMES):
        flat = active_ref[t].reshape(2 * W, C).astype(F32)
        turn_ref[:, t * 2 * W : (t + 1) * 2 * W] = keep_first(core, flat.T).astype(BF)

    def body(i, carry):
        for j in range(3):
            for k in range(3):
                rhs = jnp.concatenate(
                    [across_ref[k, t + 2 - i, (2 - j) * W : (4 - j) * W] for t in range(FRAMES)], axis=0
                )
                product = jnp.dot(turn_ref[...], rhs, preferred_element_type=F32)
                put_tap(keep_ref, send_ref, i * 9 + j * 3 + k, product)
        return carry

    lax.fori_loop(0, 3, body, 0)


def first_grad_kernel(
    core_ref, grad_ref, own_ref, rows_ref, time_ref, keep_ref, send_ref, ext_ref, across_ref, turn_ref
):
    core = core_ref[0]
    fill_ext(ext_ref, own_ref, rows_ref, time_ref, 2, 0)
    for t in range(FRAMES):
        for k, copy in enumerate(shift_copies(grad_ref[t].reshape(2 * W, C))):
            across_ref[k, t * 2 * W : (t + 1) * 2 * W] = copy
    for f in range(EXT):
        turn_ref[f] = keep_first(core, ext_ref[f].astype(F32).T).astype(BF)

    def body(i, carry):
        for j in range(3):
            lhs = jnp.concatenate(
                [turn_ref[t + i, :, j * W : (j + 2) * W] for t in range(FRAMES)], axis=1
            )
            for k in range(3):
                product = jnp.dot(lhs, across_ref[k], preferred_element_type=F32)
                put_tap(keep_ref, send_ref, i * 9 + j * 3 + k, product)
        return carry

    lax.fori_loop(0, 3, body, 0)


def cost(flops, moved):
    return pl.CostEstimate(flops=flops, bytes_accessed=moved, transcendentals=0)


def whole(kernel, outs, scratch, limit, smem=0, hbm=(), flops=PASS_FLOPS):
    def call(*args):
        moved = sum(a.size * a.dtype.itemsize for a in args)
        moved += sum(o.size * o.dtype.itemsize for o in outs)
        spaces = [
            pltpu.SMEM if n < smem else pltpu.HBM if n in hbm else pltpu.VMEM for n in range(len(args))
        ]
        return pl.pallas_call(
            kernel,
            out_shape=outs,
            in_specs=[pl.BlockSpec(memory_space=space) for space in spaces],
            out_specs=[pl.BlockSpec(memory_space=pltpu.VMEM) for _ in outs],
            scratch_shapes=scratch,
            compiler_params=pltpu.CompilerParams(vmem_limit_bytes=limit << 20),
            cost_estimate=cost(flops, moved),
        )(*args)

    return call


def convolution(kernel, outs):
    scratch = [
        pltpu.VMEM((EXT, 4 * W, C), BF),
        pltpu.VMEM((3, 9, C, C), BF),
        pltpu.SemaphoreType.DMA((3,)),
    ]
    return whole(kernel, outs, scratch, 24, hbm=(3,))


STEP = 3


def assemble_kernel(core_ref, own_ref, far_ref, first_ref, second_ref):
    core = core_ref[0]
    start = pl.program_id(0) * STEP
    mine = pl.multiple_of(core * 128, 128)
    theirs = pl.multiple_of((1 - core) * 128, 128)
    for grad, out in ((0, second_ref), (1, first_ref)):
        for p in range(STEP):
            for b in range(2):
                lanes = slice(b * 128, (b + 1) * 128)
                for rows, ref in ((mine, own_ref), (theirs, far_ref)):
                    half = ref[grad, :, b, start + p].astype(F32)
                    out[p, pl.ds(rows, 128), lanes] = half.reshape(128, 128)


def assemble(core, own, far):
    own, far = (v.reshape(2, 16, 2, TAPS, 8, 128) for v in (own, far))
    out = pl.BlockSpec((STEP, C, C), lambda p: (p, 0, 0))
    shape = jax.ShapeDtypeStruct((TAPS, C, C), F32)
    whole_array = pl.BlockSpec(memory_space=pltpu.VMEM)
    return pl.pallas_call(
        assemble_kernel,
        out_shape=(shape, shape),
        grid=(TAPS // STEP,),
        in_specs=[pl.BlockSpec(memory_space=pltpu.SMEM), whole_array, whole_array],
        out_specs=(out, out),
        compiler_params=pltpu.CompilerParams(vmem_limit_bytes=24 << 20),
        cost_estimate=cost(1 << 24, 28 << 20),
        name="assemble",
    )(core, own, far)


def total_kernel(parts_ref, out_ref):
    def body(q, carry):
        value = parts_ref[0, q].astype(F32)
        for n in range(1, parts_ref.shape[0]):
            value = value + parts_ref[n, q].astype(F32)
        rounded = value.astype(BF)
        for n in range(out_ref.shape[0]):
            out_ref[n, q] = rounded
        return carry

    lax.fori_loop(0, parts_ref.shape[1], body, 0)


def total(parts, copies):
    shape = jax.ShapeDtypeStruct((copies, *parts.shape[1:]), BF)
    return whole(total_kernel, (shape,), [], 16, flops=1 << 28)(parts)[0]


def stage_groups():
    sizes = [lax.axis_size(axis) for axis in ALL]
    grid = np.arange(math.prod(sizes)).reshape(sizes)
    stages = []
    for order in ("xy", "yz", "zx"):
        groups = []
        for core, axis in enumerate(order):
            chips = grid[:, core]
            chips = {
                "x": chips,
                "y": np.moveaxis(chips, 2, -1),
                "z": np.moveaxis(chips, (0, 1), (-2, -1)),
            }[axis]
            groups += chips.reshape(-1, 4).tolist()
        stages.append(groups)
    return stages


def exchange(value, groups):
    return lax.all_to_all(value, ALL, 0, 0, axis_index_groups=groups, tiled=False)


def swap(value, axis, steps):
    count = lax.axis_size(axis)
    pairs = [(n, n + steps) for n in range(count) if 0 <= n + steps < count]
    return lax.ppermute(value, axis, pairs)


def edge_rows(one, two):
    to_above = jnp.stack([one[:, 0], two[:, 0]])
    to_below = jnp.stack([one[:, 1], two[:, 1]])
    above = swap(to_below, SPACE, 1)
    below = swap(to_above, SPACE, -1)
    return jnp.stack([above, below])


def two_frames(own, rows, which, start):
    frames = slice(start, start + 2)
    return jnp.concatenate(
        [rows[0, which, frames][:, None], own[frames], rows[1, which, frames][:, None]], axis=1
    )


def step(latents, first_kernel, second_kernel, upstream):
    core = lax.axis_index("co").astype(jnp.int32).reshape(1)
    k1 = first_kernel.reshape(9, 3, C, C)
    k2 = second_kernel.reshape(9, 3, C, C)
    wide = latents.astype(F32)
    smooth = (wide * jax.nn.sigmoid(wide)).astype(BF)
    block = jax.ShapeDtypeStruct((FRAMES, 2, W, C), BF)
    ext = pltpu.VMEM((EXT, 4 * W, C), BF)

    rows = edge_rows(smooth, upstream)
    smooth_time = swap(two_frames(smooth, rows, 0, 2), GROUP, 1)
    up_time = swap(two_frames(upstream, rows, 1, 0), GROUP, -1)
    hidden, active = convolution(
        hidden_kernel, (jax.ShapeDtypeStruct((FRAMES, 2 * W, C), F32), block)
    )(smooth, rows, smooth_time, k1)
    (hidden_grad,) = convolution(hidden_grad_kernel, (block,))(
        upstream, rows, up_time, k2, hidden
    )

    late = edge_rows(active, hidden_grad)
    active_time = swap(two_frames(active, late, 0, 2), GROUP, 1)
    grad_time = swap(two_frames(hidden_grad, late, 1, 0), GROUP, -1)

    half = (16, 2, TAPS, 8, 128)
    pair = (jax.ShapeDtypeStruct(half, F32), jax.ShapeDtypeStruct(half, BF))
    keep2, send2 = whole(
        second_grad_kernel, pair, [ext, pltpu.VMEM((3, EXT, 4 * W, C), BF), pltpu.VMEM((C, FRAMES * 2 * W), BF)], 40, 1
    )(core, active, upstream, rows, up_time)
    keep1, send1 = whole(
        first_grad_kernel, pair, [ext, pltpu.VMEM((3, FRAMES * 2 * W, C), BF), pltpu.VMEM((EXT, C, 4 * W), BF)], 40, 1
    )(core, hidden_grad, smooth, rows, smooth_time)

    across = [(0, 1), (1, 0)]
    got2 = lax.ppermute(send2, "co", across)
    got1 = lax.ppermute(send1, "co", across)
    mine = jnp.stack([(keep2 + got2.astype(F32)).astype(BF), (keep1 + got1.astype(F32)).astype(BF)])
    stages = stage_groups()
    parts = exchange(mine.reshape(4, 16, TAPS, 8, 128), stages[0])
    held = total(parts, 1)
    parts = exchange(held.reshape(4, 4, TAPS, 8, 128), stages[1])
    parts = exchange(total(parts, 1).reshape(4, 1, TAPS, 8, 128), stages[2])
    held = exchange(total(parts, 4), stages[2])
    for groups in stages[1::-1]:
        spread = jnp.broadcast_to(held.reshape(1, -1, TAPS, 8, 128), (4, held.size // (TAPS * 1024), TAPS, 8, 128))
        held = exchange(spread, groups)
    own = held
    far = lax.ppermute(own, "co", across)

    (decoded,) = convolution(decoded_kernel, (block,))(
        active, late, active_time, k2, latents
    )
    (latent_grad,) = convolution(latent_grad_kernel, (block,))(hidden_grad, late, grad_time, k1, latents, upstream)
    first_grad, second_grad = assemble(core, own, far)
    shape = first_kernel.shape
    return (decoded, latent_grad, first_grad.reshape(shape), second_grad.reshape(shape))


def solution(mesh, sizes=(2, 2, 2, 4, 4)):
    fine = Mesh(mesh.devices.reshape(sizes), ("zl", "co", "zh", "y", "x"))
    placed = (P(GROUP, SPACE, None, None), P(), P(), P(GROUP, SPACE, None, None))
    return jax.shard_map(
        step,
        mesh=fine,
        in_specs=placed,
        out_specs=(P(GROUP, SPACE, None, None), P(GROUP, SPACE, None, None), P(), P()),
        check_vma=False,
    )
```

```python
import math

import jax
import jax.numpy as jnp
import numpy as np
from jax import lax
from jax.experimental import pallas as pl
from jax.experimental.pallas import tpu as pltpu
from jax.sharding import Mesh, PartitionSpec as P


GROUP = ("zl", "co")
SPACE = ("zh", "y", "x")
ALL = ("zl", "co", "zh", "y", "x")
C = 256
W = 128
FRAMES = 4
EXT = FRAMES + 2
TAPS = 27
BF = jnp.bfloat16
F32 = jnp.float32
PASS_FLOPS = 2 * FRAMES * 2 * W * TAPS * C * C


def fill_ext(ext_ref, own_ref, above_ref, below_ref, time_ref, first, which=0):
    other = 0 if first == 2 else FRAMES
    for f in range(FRAMES):
        ext_ref[first + f, 0:W] = above_ref[which, f]
        for r in range(2):
            ext_ref[first + f, (r + 1) * W : (r + 2) * W] = own_ref[f, r]
        ext_ref[first + f, 3 * W : 4 * W] = below_ref[which, f]
    for f in range(2):
        for r in range(4):
            ext_ref[other + f, r * W : (r + 1) * W] = time_ref[f, r]


def shifted(value, by):
    height = value.shape[0]
    turned = pltpu.roll(value, by % height, 0)
    column = lax.broadcasted_iota(jnp.int32, value.shape, 0) % W
    edge = 0 if by > 0 else W - 1
    return jnp.where(column == edge, 0.0, turned)


def conv_frame(ext_ref, kernel_ref, t, transposed):
    parts = []
    for i in range(3):
        for j in range(3):
            frame = t + (2 - i if transposed else i)
            row = 2 - j if transposed else j
            parts.append(ext_ref[frame, row * W : (row + 2) * W])
    lhs = jnp.concatenate(parts, axis=1)
    sums = []
    for k in range(3):
        taps = [kernel_ref[k, n] for n in range(9)]
        if transposed:
            rhs = jnp.concatenate(taps, axis=1)
            dims = (((1,), (1,)), ((), ()))
        else:
            rhs = jnp.concatenate(taps, axis=0)
            dims = (((1,), (0,)), ((), ()))
        sums.append(lax.dot_general(lhs, rhs, dims, preferred_element_type=F32))
    if transposed:
        return sums[1] + shifted(sums[0], -1) + shifted(sums[2], 1)
    return sums[1] + shifted(sums[0], 1) + shifted(sums[2], -1)


def gate_grad(values):
    s = jax.nn.sigmoid(values)
    return s * (1.0 + values * (1.0 - s))


def load_taps(source_ref, kernel_ref, sem):
    copies = [
        pltpu.make_async_copy(source_ref.at[:, k], kernel_ref.at[k], sem.at[k]) for k in range(3)
    ]
    for copy in copies:
        copy.start()
    return copies


def split_rows(value):
    return value.reshape(2, W, C)


def hidden_kernel(own_ref, above_ref, below_ref, time_ref, source_ref, hidden_ref, active_ref, ext_ref, kernel_ref, sem):
    copies = load_taps(source_ref, kernel_ref, sem)
    fill_ext(ext_ref, own_ref, above_ref, below_ref, time_ref, 2)
    for copy in copies:
        copy.wait()

    def body(t, carry):
        hidden = conv_frame(ext_ref, kernel_ref, t, False)
        hidden_ref[t] = hidden
        active_ref[t] = split_rows((hidden * jax.nn.sigmoid(hidden)).astype(BF))
        return carry

    lax.fori_loop(0, FRAMES, body, 0)


def hidden_grad_kernel(own_ref, above_ref, below_ref, time_ref, source_ref, hidden_ref, out_ref, ext_ref, kernel_ref, sem):
    copies = load_taps(source_ref, kernel_ref, sem)
    fill_ext(ext_ref, own_ref, above_ref, below_ref, time_ref, 0)
    for copy in copies:
        copy.wait()

    def body(t, carry):
        grad = conv_frame(ext_ref, kernel_ref, t, True)
        out_ref[t] = split_rows((grad * gate_grad(hidden_ref[t])).astype(BF))
        return carry

    lax.fori_loop(0, FRAMES, body, 0)


def decoded_kernel(own_ref, above_ref, below_ref, time_ref, source_ref, latents_ref, out_ref, ext_ref, kernel_ref, sem):
    copies = load_taps(source_ref, kernel_ref, sem)
    fill_ext(ext_ref, own_ref, above_ref, below_ref, time_ref, 2, 0)
    for copy in copies:
        copy.wait()

    def body(t, carry):
        branch = split_rows(conv_frame(ext_ref, kernel_ref, t, False))
        out_ref[t] = (latents_ref[t].astype(F32) + branch).astype(BF)
        return carry

    lax.fori_loop(0, FRAMES, body, 0)


def latent_grad_kernel(
    own_ref, above_ref, below_ref, time_ref, source_ref, latents_ref, upstream_ref, out_ref, ext_ref, kernel_ref, sem
):
    copies = load_taps(source_ref, kernel_ref, sem)
    fill_ext(ext_ref, own_ref, above_ref, below_ref, time_ref, 0, 1)
    for copy in copies:
        copy.wait()

    def body(t, carry):
        inner = split_rows(conv_frame(ext_ref, kernel_ref, t, True))
        gate = gate_grad(latents_ref[t].astype(F32))
        out_ref[t] = (upstream_ref[t].astype(F32) + inner * gate).astype(BF)
        return carry

    lax.fori_loop(0, FRAMES, body, 0)


def keep_first(core, value):
    return jnp.where(core == 0, value, pltpu.roll(value, C // 2, 0))


def shift_copies(value):
    wide = value.astype(F32)
    return [shifted(wide, -1).astype(BF), value, shifted(wide, 1).astype(BF)]


def put_tap(keep_ref, send_ref, tap, product):
    for ref, low in ((keep_ref, 0), (send_ref, C // 2)):
        half = product[low : low + C // 2].astype(ref.dtype)
        for b in range(2):
            ref[:, b, tap] = half[:, b * 128 : (b + 1) * 128].reshape(16, 8, 128)


def second_grad_kernel(
    core_ref, active_ref, own_ref, above_ref, below_ref, time_ref, keep_ref, send_ref, ext_ref, across_ref, turn_ref
):
    core = core_ref[0]
    fill_ext(ext_ref, own_ref, above_ref, below_ref, time_ref, 0)
    for f in range(EXT):
        for k, copy in enumerate(shift_copies(ext_ref[f])):
            across_ref[k, f] = copy
    for t in range(FRAMES):
        flat = active_ref[t].reshape(2 * W, C).astype(F32)
        turn_ref[:, t * 2 * W : (t + 1) * 2 * W] = keep_first(core, flat.T).astype(BF)

    def body(i, carry):
        for j in range(3):
            for k in range(3):
                rhs = jnp.concatenate(
                    [across_ref[k, t + 2 - i, (2 - j) * W : (4 - j) * W] for t in range(FRAMES)], axis=0
                )
                product = jnp.dot(turn_ref[...], rhs, preferred_element_type=F32)
                put_tap(keep_ref, send_ref, i * 9 + j * 3 + k, product)
        return carry

    lax.fori_loop(0, 3, body, 0)


def first_grad_kernel(
    core_ref, grad_ref, own_ref, above_ref, below_ref, time_ref, keep_ref, send_ref, ext_ref, across_ref, turn_ref
):
    core = core_ref[0]
    fill_ext(ext_ref, own_ref, above_ref, below_ref, time_ref, 2)
    for t in range(FRAMES):
        for k, copy in enumerate(shift_copies(grad_ref[t].reshape(2 * W, C))):
            across_ref[k, t * 2 * W : (t + 1) * 2 * W] = copy
    for f in range(EXT):
        turn_ref[f] = keep_first(core, ext_ref[f].astype(F32).T).astype(BF)

    def body(i, carry):
        for j in range(3):
            lhs = jnp.concatenate(
                [turn_ref[t + i, :, j * W : (j + 2) * W] for t in range(FRAMES)], axis=1
            )
            for k in range(3):
                product = jnp.dot(lhs, across_ref[k], preferred_element_type=F32)
                put_tap(keep_ref, send_ref, i * 9 + j * 3 + k, product)
        return carry

    lax.fori_loop(0, 3, body, 0)


def cost(flops, moved):
    return pl.CostEstimate(flops=flops, bytes_accessed=moved, transcendentals=0)


def whole(kernel, outs, scratch, limit, smem=0, hbm=(), flops=PASS_FLOPS):
    def call(*args):
        moved = sum(a.size * a.dtype.itemsize for a in args)
        moved += sum(o.size * o.dtype.itemsize for o in outs)
        spaces = [
            pltpu.SMEM if n < smem else pltpu.HBM if n in hbm else pltpu.VMEM for n in range(len(args))
        ]
        return pl.pallas_call(
            kernel,
            out_shape=outs,
            in_specs=[pl.BlockSpec(memory_space=space) for space in spaces],
            out_specs=[pl.BlockSpec(memory_space=pltpu.VMEM) for _ in outs],
            scratch_shapes=scratch,
            compiler_params=pltpu.CompilerParams(vmem_limit_bytes=limit << 20),
            cost_estimate=cost(flops, moved),
        )(*args)

    return call


def convolution(kernel, outs):
    scratch = [
        pltpu.VMEM((EXT, 4 * W, C), BF),
        pltpu.VMEM((3, 9, C, C), BF),
        pltpu.SemaphoreType.DMA((3,)),
    ]
    return whole(kernel, outs, scratch, 24, hbm=(4,))


STEP = 3


def assemble_kernel(core_ref, own_ref, far_ref, first_ref, second_ref):
    core = core_ref[0]
    start = pl.program_id(0) * STEP
    mine = pl.multiple_of(core * 128, 128)
    theirs = pl.multiple_of((1 - core) * 128, 128)
    for grad, out in ((0, second_ref), (1, first_ref)):
        for p in range(STEP):
            for b in range(2):
                lanes = slice(b * 128, (b + 1) * 128)
                for rows, ref in ((mine, own_ref), (theirs, far_ref)):
                    half = ref[grad, :, b, start + p].astype(F32)
                    out[p, pl.ds(rows, 128), lanes] = half.reshape(128, 128)


def assemble(core, own, far):
    own, far = (v.reshape(2, 16, 2, TAPS, 8, 128) for v in (own, far))
    out = pl.BlockSpec((STEP, C, C), lambda p: (p, 0, 0))
    shape = jax.ShapeDtypeStruct((TAPS, C, C), F32)
    whole_array = pl.BlockSpec(memory_space=pltpu.VMEM)
    return pl.pallas_call(
        assemble_kernel,
        out_shape=(shape, shape),
        grid=(TAPS // STEP,),
        in_specs=[pl.BlockSpec(memory_space=pltpu.SMEM), whole_array, whole_array],
        out_specs=(out, out),
        compiler_params=pltpu.CompilerParams(vmem_limit_bytes=24 << 20),
        cost_estimate=cost(1 << 24, 28 << 20),
        name="assemble",
    )(core, own, far)


def total_kernel(parts_ref, out_ref):
    def body(q, carry):
        value = parts_ref[0, q].astype(F32)
        for n in range(1, parts_ref.shape[0]):
            value = value + parts_ref[n, q].astype(F32)
        rounded = value.astype(BF)
        for n in range(out_ref.shape[0]):
            out_ref[n, q] = rounded
        return carry

    lax.fori_loop(0, parts_ref.shape[1], body, 0)


def total(parts, copies):
    shape = jax.ShapeDtypeStruct((copies, *parts.shape[1:]), BF)
    return whole(total_kernel, (shape,), [], 16, flops=1 << 28)(parts)[0]


def stage_groups():
    sizes = [lax.axis_size(axis) for axis in ALL]
    grid = np.arange(math.prod(sizes)).reshape(sizes)
    near, rest = ([], [])
    for core, axis in ((0, 3), (1, 2)):
        chips = np.moveaxis(grid[:, core], axis, -1)
        lines = chips.reshape(-1, chips.shape[-1])
        near += lines.tolist()
        rest += lines.T.tolist()
    return near, rest


def exchange(value, groups):
    return lax.all_to_all(value, ALL, 0, 0, axis_index_groups=groups, tiled=False)


def swap(value, axis, steps):
    count = lax.axis_size(axis)
    pairs = [(n, n + steps) for n in range(count) if 0 <= n + steps < count]
    return lax.ppermute(value, axis, pairs)


def edge_rows(arrays):
    above = swap(jnp.stack([value[:, 1] for value in arrays]), SPACE, 1)
    below = swap(jnp.stack([value[:, 0] for value in arrays]), SPACE, -1)
    return above, below


def two_frames(own, rows, which, start):
    frames = slice(start, start + 2)
    above, below = rows
    return jnp.concatenate(
        [above[which, frames][:, None], own[frames], below[which, frames][:, None]], axis=1
    )


def step(latents, first_kernel, second_kernel, upstream):
    core = lax.axis_index("co").astype(jnp.int32).reshape(1)
    k1 = first_kernel.reshape(9, 3, C, C)
    k2 = second_kernel.reshape(9, 3, C, C)
    wide = latents.astype(F32)
    smooth = (wide * jax.nn.sigmoid(wide)).astype(BF)
    block = jax.ShapeDtypeStruct((FRAMES, 2, W, C), BF)
    ext = pltpu.VMEM((EXT, 4 * W, C), BF)

    rows = edge_rows((smooth,))
    up_rows = edge_rows((upstream,))
    smooth_time = swap(two_frames(smooth, rows, 0, 2), GROUP, 1)
    up_time = swap(two_frames(upstream, up_rows, 0, 0), GROUP, -1)
    hidden, active = convolution(
        hidden_kernel, (jax.ShapeDtypeStruct((FRAMES, 2 * W, C), F32), block)
    )(smooth, *rows, smooth_time, k1)
    (hidden_grad,) = convolution(hidden_grad_kernel, (block,))(
        upstream, *up_rows, up_time, k2, hidden
    )

    late = edge_rows((active, hidden_grad))
    half = (16, 2, TAPS, 8, 128)
    pair = (jax.ShapeDtypeStruct(half, F32), jax.ShapeDtypeStruct(half, BF))
    keep2, send2 = whole(
        second_grad_kernel, pair, [ext, pltpu.VMEM((3, EXT, 4 * W, C), BF), pltpu.VMEM((C, FRAMES * 2 * W), BF)], 40, 1
    )(core, active, upstream, *up_rows, up_time)
    keep1, send1 = whole(
        first_grad_kernel, pair, [ext, pltpu.VMEM((3, FRAMES * 2 * W, C), BF), pltpu.VMEM((EXT, C, 4 * W), BF)], 40, 1
    )(core, hidden_grad, smooth, *rows, smooth_time)

    across = [(0, 1), (1, 0)]
    got2 = lax.ppermute(send2, "co", across)
    got1 = lax.ppermute(send1, "co", across)
    mine = jnp.stack([(keep2 + got2.astype(F32)).astype(BF), (keep1 + got1.astype(F32)).astype(BF)])
    near, rest = stage_groups()
    first, second = (len(near[0]), len(rest[0]))
    block_rows = 64 // (first * second) * TAPS
    parts = exchange(mine.reshape(first, second, block_rows, 8, 128), near)
    quarter = total(parts, 1)
    active_own, grad_own, _ = lax.optimization_barrier((active, hidden_grad, quarter))
    active_time = swap(two_frames(active_own, late, 0, 2), GROUP, 1)
    grad_time = swap(two_frames(grad_own, late, 1, 0), GROUP, -1)
    parts = exchange(quarter.reshape(second, block_rows, 8, 128), rest)
    spread = total(parts[:, None], second)
    quarter = exchange(spread.reshape(second, block_rows, 8, 128), rest)
    own = exchange(jnp.broadcast_to(quarter[None], (first, *quarter.shape)), near)
    far = lax.ppermute(own, "co", across)

    (decoded,) = convolution(decoded_kernel, (block,))(
        active, *late, active_time, k2, latents
    )
    (latent_grad,) = convolution(latent_grad_kernel, (block,))(hidden_grad, *late, grad_time, k1, latents, upstream)
    first_grad, second_grad = assemble(core, own, far)
    shape = first_kernel.shape
    return (decoded, latent_grad, first_grad.reshape(shape), second_grad.reshape(shape))


def solution(mesh, sizes=(2, 2, 2, 4, 4)):
    fine = Mesh(mesh.devices.reshape(sizes), ("zl", "co", "zh", "y", "x"))
    placed = (P(GROUP, SPACE, None, None), P(), P(), P(GROUP, SPACE, None, None))
    return jax.shard_map(
        step,
        mesh=fine,
        in_specs=placed,
        out_specs=(P(GROUP, SPACE, None, None), P(GROUP, SPACE, None, None), P(), P()),
        check_vma=False,
    )
```

```python
import math

import jax
import jax.numpy as jnp
import numpy as np
from jax import lax
from jax.experimental import pallas as pl
from jax.experimental.pallas import tpu as pltpu
from jax.sharding import Mesh, PartitionSpec as P


GROUP = ("zl", "co")
SPACE = ("zh", "y", "x")
ALL = ("zl", "co", "zh", "y", "x")
C = 256
W = 128
FRAMES = 4
EXT = FRAMES + 2
TAPS = 27
BF = jnp.bfloat16
F32 = jnp.float32
PASS_FLOPS = 2 * FRAMES * 2 * W * TAPS * C * C


def fill_ext(ext_ref, own_ref, rows_ref, time_ref, first, which):
    other = 0 if first == 2 else FRAMES
    for f in range(FRAMES):
        ext_ref[first + f, 0:W] = rows_ref[0, which, f]
        for r in range(2):
            ext_ref[first + f, (r + 1) * W : (r + 2) * W] = own_ref[f, r]
        ext_ref[first + f, 3 * W : 4 * W] = rows_ref[1, which, f]
    for f in range(2):
        for r in range(4):
            ext_ref[other + f, r * W : (r + 1) * W] = time_ref[f, r]


def shifted(value, by):
    height = value.shape[0]
    turned = pltpu.roll(value, by % height, 0)
    column = lax.broadcasted_iota(jnp.int32, value.shape, 0) % W
    edge = 0 if by > 0 else W - 1
    return jnp.where(column == edge, 0.0, turned)


def conv_frame(ext_ref, kernel_ref, t, transposed):
    parts = []
    for i in range(3):
        for j in range(3):
            frame = t + (2 - i if transposed else i)
            row = 2 - j if transposed else j
            parts.append(ext_ref[frame, row * W : (row + 2) * W])
    lhs = jnp.concatenate(parts, axis=1)
    sums = []
    for k in range(3):
        taps = [kernel_ref[k, n] for n in range(9)]
        if transposed:
            rhs = jnp.concatenate(taps, axis=1)
            dims = (((1,), (1,)), ((), ()))
        else:
            rhs = jnp.concatenate(taps, axis=0)
            dims = (((1,), (0,)), ((), ()))
        sums.append(lax.dot_general(lhs, rhs, dims, preferred_element_type=F32))
    if transposed:
        return sums[1] + shifted(sums[0], -1) + shifted(sums[2], 1)
    return sums[1] + shifted(sums[0], 1) + shifted(sums[2], -1)


def gate_grad(values):
    s = jax.nn.sigmoid(values)
    return s * (1.0 + values * (1.0 - s))


def load_taps(source_ref, kernel_ref, sem):
    copies = [
        pltpu.make_async_copy(source_ref.at[:, k], kernel_ref.at[k], sem.at[k]) for k in range(3)
    ]
    for copy in copies:
        copy.start()
    return copies


def split_rows(value):
    return value.reshape(2, W, C)


def hidden_kernel(own_ref, rows_ref, time_ref, source_ref, hidden_ref, active_ref, ext_ref, kernel_ref, sem):
    copies = load_taps(source_ref, kernel_ref, sem)
    fill_ext(ext_ref, own_ref, rows_ref, time_ref, 2, 0)
    for copy in copies:
        copy.wait()

    def body(t, carry):
        hidden = conv_frame(ext_ref, kernel_ref, t, False)
        hidden_ref[t] = hidden
        active_ref[t] = split_rows((hidden * jax.nn.sigmoid(hidden)).astype(BF))
        return carry

    lax.fori_loop(0, FRAMES, body, 0)


def hidden_grad_kernel(own_ref, rows_ref, time_ref, source_ref, hidden_ref, out_ref, ext_ref, kernel_ref, sem):
    copies = load_taps(source_ref, kernel_ref, sem)
    fill_ext(ext_ref, own_ref, rows_ref, time_ref, 0, 1)
    for copy in copies:
        copy.wait()

    def body(t, carry):
        grad = conv_frame(ext_ref, kernel_ref, t, True)
        out_ref[t] = split_rows((grad * gate_grad(hidden_ref[t])).astype(BF))
        return carry

    lax.fori_loop(0, FRAMES, body, 0)


def decoded_kernel(own_ref, rows_ref, time_ref, source_ref, latents_ref, out_ref, ext_ref, kernel_ref, sem):
    copies = load_taps(source_ref, kernel_ref, sem)
    fill_ext(ext_ref, own_ref, rows_ref, time_ref, 2, 0)
    for copy in copies:
        copy.wait()

    def body(t, carry):
        branch = split_rows(conv_frame(ext_ref, kernel_ref, t, False))
        out_ref[t] = (latents_ref[t].astype(F32) + branch).astype(BF)
        return carry

    lax.fori_loop(0, FRAMES, body, 0)


def latent_grad_kernel(
    own_ref, rows_ref, time_ref, source_ref, latents_ref, upstream_ref, out_ref, ext_ref, kernel_ref, sem
):
    copies = load_taps(source_ref, kernel_ref, sem)
    fill_ext(ext_ref, own_ref, rows_ref, time_ref, 0, 1)
    for copy in copies:
        copy.wait()

    def body(t, carry):
        inner = split_rows(conv_frame(ext_ref, kernel_ref, t, True))
        gate = gate_grad(latents_ref[t].astype(F32))
        out_ref[t] = (upstream_ref[t].astype(F32) + inner * gate).astype(BF)
        return carry

    lax.fori_loop(0, FRAMES, body, 0)


def keep_first(core, value):
    return jnp.where(core == 0, value, pltpu.roll(value, C // 2, 0))


def shift_copies(value):
    wide = value.astype(F32)
    return [shifted(wide, -1).astype(BF), value, shifted(wide, 1).astype(BF)]


def put_tap(keep_ref, send_ref, tap, product):
    for ref, low in ((keep_ref, 0), (send_ref, C // 2)):
        half = product[low : low + C // 2].astype(ref.dtype)
        for b in range(2):
            ref[:, b, tap] = half[:, b * 128 : (b + 1) * 128].reshape(16, 8, 128)


def second_grad_kernel(
    core_ref, active_ref, own_ref, rows_ref, time_ref, keep_ref, send_ref, ext_ref, across_ref, turn_ref
):
    core = core_ref[0]
    fill_ext(ext_ref, own_ref, rows_ref, time_ref, 0, 1)
    for f in range(EXT):
        for k, copy in enumerate(shift_copies(ext_ref[f])):
            across_ref[k, f] = copy
    for t in range(FRAMES):
        flat = active_ref[t].reshape(2 * W, C).astype(F32)
        turn_ref[:, t * 2 * W : (t + 1) * 2 * W] = keep_first(core, flat.T).astype(BF)

    def body(i, carry):
        for j in range(3):
            for k in range(3):
                rhs = jnp.concatenate(
                    [across_ref[k, t + 2 - i, (2 - j) * W : (4 - j) * W] for t in range(FRAMES)], axis=0
                )
                product = jnp.dot(turn_ref[...], rhs, preferred_element_type=F32)
                put_tap(keep_ref, send_ref, i * 9 + j * 3 + k, product)
        return carry

    lax.fori_loop(0, 3, body, 0)


def first_grad_kernel(
    core_ref, grad_ref, own_ref, rows_ref, time_ref, keep_ref, send_ref, ext_ref, across_ref, turn_ref
):
    core = core_ref[0]
    fill_ext(ext_ref, own_ref, rows_ref, time_ref, 2, 0)
    for t in range(FRAMES):
        for k, copy in enumerate(shift_copies(grad_ref[t].reshape(2 * W, C))):
            across_ref[k, t * 2 * W : (t + 1) * 2 * W] = copy
    for f in range(EXT):
        turn_ref[f] = keep_first(core, ext_ref[f].astype(F32).T).astype(BF)

    def body(i, carry):
        for j in range(3):
            lhs = jnp.concatenate(
                [turn_ref[t + i, :, j * W : (j + 2) * W] for t in range(FRAMES)], axis=1
            )
            for k in range(3):
                product = jnp.dot(lhs, across_ref[k], preferred_element_type=F32)
                put_tap(keep_ref, send_ref, i * 9 + j * 3 + k, product)
        return carry

    lax.fori_loop(0, 3, body, 0)


def cost(flops, moved):
    return pl.CostEstimate(flops=flops, bytes_accessed=moved, transcendentals=0)


def whole(kernel, outs, scratch, limit, smem=0, hbm=(), flops=PASS_FLOPS):
    def call(*args):
        moved = sum(a.size * a.dtype.itemsize for a in args)
        moved += sum(o.size * o.dtype.itemsize for o in outs)
        spaces = [
            pltpu.SMEM if n < smem else pltpu.HBM if n in hbm else pltpu.VMEM for n in range(len(args))
        ]
        return pl.pallas_call(
            kernel,
            out_shape=outs,
            in_specs=[pl.BlockSpec(memory_space=space) for space in spaces],
            out_specs=[pl.BlockSpec(memory_space=pltpu.VMEM) for _ in outs],
            scratch_shapes=scratch,
            compiler_params=pltpu.CompilerParams(vmem_limit_bytes=limit << 20),
            cost_estimate=cost(flops, moved),
        )(*args)

    return call


def convolution(kernel, outs):
    scratch = [
        pltpu.VMEM((EXT, 4 * W, C), BF),
        pltpu.VMEM((3, 9, C, C), BF),
        pltpu.SemaphoreType.DMA((3,)),
    ]
    return whole(kernel, outs, scratch, 24, hbm=(3,))


STEP = 3


def assemble_kernel(core_ref, own_ref, far_ref, first_ref, second_ref):
    core = core_ref[0]
    start = pl.program_id(0) * STEP
    mine = pl.multiple_of(core * 128, 128)
    theirs = pl.multiple_of((1 - core) * 128, 128)
    for grad, out in ((0, second_ref), (1, first_ref)):
        for p in range(STEP):
            for b in range(2):
                lanes = slice(b * 128, (b + 1) * 128)
                for rows, ref in ((mine, own_ref), (theirs, far_ref)):
                    half = ref[grad, :, b, start + p].astype(F32)
                    out[p, pl.ds(rows, 128), lanes] = half.reshape(128, 128)


def assemble(core, own, far):
    own, far = (v.reshape(2, 16, 2, TAPS, 8, 128) for v in (own, far))
    out = pl.BlockSpec((STEP, C, C), lambda p: (p, 0, 0))
    shape = jax.ShapeDtypeStruct((TAPS, C, C), F32)
    whole_array = pl.BlockSpec(memory_space=pltpu.VMEM)
    return pl.pallas_call(
        assemble_kernel,
        out_shape=(shape, shape),
        grid=(TAPS // STEP,),
        in_specs=[pl.BlockSpec(memory_space=pltpu.SMEM), whole_array, whole_array],
        out_specs=(out, out),
        compiler_params=pltpu.CompilerParams(vmem_limit_bytes=24 << 20),
        cost_estimate=cost(1 << 24, 28 << 20),
        name="assemble",
    )(core, own, far)


def total_kernel(parts_ref, out_ref):
    def body(q, carry):
        value = parts_ref[0, q].astype(F32)
        for n in range(1, parts_ref.shape[0]):
            value = value + parts_ref[n, q].astype(F32)
        rounded = value.astype(BF)
        for n in range(out_ref.shape[0]):
            out_ref[n, q] = rounded
        return carry

    lax.fori_loop(0, parts_ref.shape[1], body, 0)


def total(parts, copies):
    shape = jax.ShapeDtypeStruct((copies, *parts.shape[1:]), BF)
    return whole(total_kernel, (shape,), [], 16, flops=1 << 28)(parts)[0]


def stage_groups():
    sizes = [lax.axis_size(axis) for axis in ALL]
    grid = np.arange(math.prod(sizes)).reshape(sizes)
    near, rest = ([], [])
    for core, axis in ((0, 3), (1, 2)):
        chips = np.moveaxis(grid[:, core], axis, -1)
        lines = chips.reshape(-1, chips.shape[-1])
        near += lines.tolist()
        rest += lines.T.tolist()
    return near, rest


def exchange(value, groups):
    return lax.all_to_all(value, ALL, 0, 0, axis_index_groups=groups, tiled=False)


def swap(value, axis, steps):
    count = lax.axis_size(axis)
    pairs = [(n, n + steps) for n in range(count) if 0 <= n + steps < count]
    return lax.ppermute(value, axis, pairs)


def edge_rows(one, two):
    to_above = jnp.stack([one[:, 0], two[:, 0]])
    to_below = jnp.stack([one[:, 1], two[:, 1]])
    above = swap(to_below, SPACE, 1)
    below = swap(to_above, SPACE, -1)
    return jnp.stack([above, below])


def two_frames(own, rows, which, start):
    frames = slice(start, start + 2)
    return jnp.concatenate(
        [rows[0, which, frames][:, None], own[frames], rows[1, which, frames][:, None]], axis=1
    )


def step(latents, first_kernel, second_kernel, upstream):
    core = lax.axis_index("co").astype(jnp.int32).reshape(1)
    k1 = first_kernel.reshape(9, 3, C, C)
    k2 = second_kernel.reshape(9, 3, C, C)
    wide = latents.astype(F32)
    smooth = (wide * jax.nn.sigmoid(wide)).astype(BF)
    block = jax.ShapeDtypeStruct((FRAMES, 2, W, C), BF)
    ext = pltpu.VMEM((EXT, 4 * W, C), BF)

    rows = edge_rows(smooth, upstream)
    smooth_time = swap(two_frames(smooth, rows, 0, 2), GROUP, 1)
    up_time = swap(two_frames(upstream, rows, 1, 0), GROUP, -1)
    hidden, active = convolution(
        hidden_kernel, (jax.ShapeDtypeStruct((FRAMES, 2 * W, C), F32), block)
    )(smooth, rows, smooth_time, pltpu.with_memory_space_constraint(k1, pltpu.HBM))
    (hidden_grad,) = convolution(hidden_grad_kernel, (block,))(
        upstream, rows, up_time, k2, hidden
    )

    late = edge_rows(active, hidden_grad)
    active_time = swap(two_frames(active, late, 0, 2), GROUP, 1)
    grad_time = swap(two_frames(hidden_grad, late, 1, 0), GROUP, -1)

    half = (16, 2, TAPS, 8, 128)
    pair = (jax.ShapeDtypeStruct(half, F32), jax.ShapeDtypeStruct(half, BF))
    keep2, send2 = whole(
        second_grad_kernel, pair, [ext, pltpu.VMEM((3, EXT, 4 * W, C), BF), pltpu.VMEM((C, FRAMES * 2 * W), BF)], 40, 1
    )(core, active, upstream, rows, up_time)
    keep1, send1 = whole(
        first_grad_kernel, pair, [ext, pltpu.VMEM((3, FRAMES * 2 * W, C), BF), pltpu.VMEM((EXT, C, 4 * W), BF)], 40, 1
    )(core, hidden_grad, smooth, rows, smooth_time)

    across = [(0, 1), (1, 0)]
    got2 = lax.ppermute(send2, "co", across)
    got1 = lax.ppermute(send1, "co", across)
    mine = jnp.stack([(keep2 + got2.astype(F32)).astype(BF), (keep1 + got1.astype(F32)).astype(BF)])
    near, rest = stage_groups()
    first, second = (len(near[0]), len(rest[0]))
    block_rows = 64 // (first * second) * TAPS
    parts = exchange(mine.reshape(first, second, block_rows, 8, 128), near)
    quarter = total(parts, 1)
    parts = exchange(quarter.reshape(second, block_rows, 8, 128), rest)
    spread = total(parts[:, None], second)
    quarter = exchange(spread.reshape(second, block_rows, 8, 128), rest)
    own = exchange(jnp.broadcast_to(quarter[None], (first, *quarter.shape)), near)
    far = lax.ppermute(own, "co", across)

    (decoded,) = convolution(decoded_kernel, (block,))(
        active, late, active_time, k2, latents
    )
    (latent_grad,) = convolution(latent_grad_kernel, (block,))(hidden_grad, late, grad_time, k1, latents, upstream)
    first_grad, second_grad = assemble(core, own, far)
    shape = first_kernel.shape
    return (decoded, latent_grad, first_grad.reshape(shape), second_grad.reshape(shape))


def solution(mesh, sizes=(2, 2, 2, 4, 4)):
    fine = Mesh(mesh.devices.reshape(sizes), ("zl", "co", "zh", "y", "x"))
    placed = (P(GROUP, SPACE, None, None), P(), P(), P(GROUP, SPACE, None, None))
    return jax.shard_map(
        step,
        mesh=fine,
        in_specs=placed,
        out_specs=(P(GROUP, SPACE, None, None), P(GROUP, SPACE, None, None), P(), P()),
        check_vma=False,
    )
```

```python
import math

import jax
import jax.numpy as jnp
import numpy as np
from jax import lax
from jax.experimental import pallas as pl
from jax.experimental.pallas import tpu as pltpu
from jax.sharding import Mesh, PartitionSpec as P


GROUP = ("zl", "co")
SPACE = ("zh", "y", "x")
ALL = ("zl", "co", "zh", "y", "x")
C = 256
W = 128
FRAMES = 4
EXT = FRAMES + 2
TAPS = 27
BF = jnp.bfloat16
F32 = jnp.float32
PASS_FLOPS = 2 * FRAMES * 2 * W * TAPS * C * C


def fill_ext(ext_ref, own_ref, rows_ref, time_ref, first, which):
    other = 0 if first == 2 else FRAMES
    for f in range(FRAMES):
        ext_ref[first + f, 0:W] = rows_ref[0, which, f]
        for r in range(2):
            ext_ref[first + f, (r + 1) * W : (r + 2) * W] = own_ref[f, r]
        ext_ref[first + f, 3 * W : 4 * W] = rows_ref[1, which, f]
    for f in range(2):
        for r in range(4):
            ext_ref[other + f, r * W : (r + 1) * W] = time_ref[f, r]


def shifted(value, by):
    height = value.shape[0]
    turned = pltpu.roll(value, by % height, 0)
    column = lax.broadcasted_iota(jnp.int32, value.shape, 0) % W
    edge = 0 if by > 0 else W - 1
    return jnp.where(column == edge, 0.0, turned)


def conv_frame(ext_ref, kernel_ref, t, transposed, copies):
    parts = []
    for i in range(3):
        for j in range(3):
            frame = t + (2 - i if transposed else i)
            row = 2 - j if transposed else j
            parts.append(ext_ref[frame, row * W : (row + 2) * W])
    lhs = jnp.concatenate(parts, axis=1)
    sums = []
    for k in range(3):
        pl.when(t == 0)(copies[k].wait)
        taps = [kernel_ref[k, n] for n in range(9)]
        if transposed:
            rhs = jnp.concatenate(taps, axis=1)
            dims = (((1,), (1,)), ((), ()))
        else:
            rhs = jnp.concatenate(taps, axis=0)
            dims = (((1,), (0,)), ((), ()))
        sums.append(lax.dot_general(lhs, rhs, dims, preferred_element_type=F32))
    if transposed:
        return sums[1] + shifted(sums[0], -1) + shifted(sums[2], 1)
    return sums[1] + shifted(sums[0], 1) + shifted(sums[2], -1)


def gate_grad(values):
    s = jax.nn.sigmoid(values)
    return s * (1.0 + values * (1.0 - s))


def load_taps(source_ref, kernel_ref, sem):
    copies = [
        pltpu.make_async_copy(source_ref.at[:, k], kernel_ref.at[k], sem.at[k]) for k in range(3)
    ]
    for copy in copies:
        copy.start()
    return copies


def split_rows(value):
    return value.reshape(2, W, C)


def hidden_kernel(own_ref, rows_ref, time_ref, source_ref, hidden_ref, active_ref, ext_ref, kernel_ref, sem):
    copies = load_taps(source_ref, kernel_ref, sem)
    fill_ext(ext_ref, own_ref, rows_ref, time_ref, 2, 0)

    def body(t, carry):
        hidden = conv_frame(ext_ref, kernel_ref, t, False, copies)
        hidden_ref[t] = hidden
        active_ref[t] = split_rows((hidden * jax.nn.sigmoid(hidden)).astype(BF))
        return carry

    lax.fori_loop(0, FRAMES, body, 0)


def hidden_grad_kernel(own_ref, rows_ref, time_ref, source_ref, hidden_ref, out_ref, ext_ref, kernel_ref, sem):
    copies = load_taps(source_ref, kernel_ref, sem)
    fill_ext(ext_ref, own_ref, rows_ref, time_ref, 0, 1)

    def body(t, carry):
        grad = conv_frame(ext_ref, kernel_ref, t, True, copies)
        out_ref[t] = split_rows((grad * gate_grad(hidden_ref[t])).astype(BF))
        return carry

    lax.fori_loop(0, FRAMES, body, 0)


def decoded_kernel(own_ref, rows_ref, time_ref, source_ref, latents_ref, out_ref, ext_ref, kernel_ref, sem):
    copies = load_taps(source_ref, kernel_ref, sem)
    fill_ext(ext_ref, own_ref, rows_ref, time_ref, 2, 0)

    def body(t, carry):
        branch = split_rows(conv_frame(ext_ref, kernel_ref, t, False, copies))
        out_ref[t] = (latents_ref[t].astype(F32) + branch).astype(BF)
        return carry

    lax.fori_loop(0, FRAMES, body, 0)


def latent_grad_kernel(
    own_ref, rows_ref, time_ref, source_ref, latents_ref, upstream_ref, out_ref, ext_ref, kernel_ref, sem
):
    copies = load_taps(source_ref, kernel_ref, sem)
    fill_ext(ext_ref, own_ref, rows_ref, time_ref, 0, 1)

    def body(t, carry):
        inner = split_rows(conv_frame(ext_ref, kernel_ref, t, True, copies))
        gate = gate_grad(latents_ref[t].astype(F32))
        out_ref[t] = (upstream_ref[t].astype(F32) + inner * gate).astype(BF)
        return carry

    lax.fori_loop(0, FRAMES, body, 0)


def keep_first(core, value):
    return jnp.where(core == 0, value, pltpu.roll(value, C // 2, 0))


def shift_copies(value):
    wide = value.astype(F32)
    return [shifted(wide, -1).astype(BF), value, shifted(wide, 1).astype(BF)]


def put_tap(keep_ref, send_ref, tap, product):
    for ref, low in ((keep_ref, 0), (send_ref, C // 2)):
        half = product[low : low + C // 2].astype(ref.dtype)
        for b in range(2):
            ref[:, b, tap] = half[:, b * 128 : (b + 1) * 128].reshape(16, 8, 128)


def second_grad_kernel(
    core_ref, active_ref, own_ref, rows_ref, time_ref, keep_ref, send_ref, ext_ref, across_ref, turn_ref
):
    core = core_ref[0]
    fill_ext(ext_ref, own_ref, rows_ref, time_ref, 0, 1)
    for f in range(EXT):
        for k, copy in enumerate(shift_copies(ext_ref[f])):
            across_ref[k, f] = copy
    for t in range(FRAMES):
        flat = active_ref[t].reshape(2 * W, C).astype(F32)
        turn_ref[:, t * 2 * W : (t + 1) * 2 * W] = keep_first(core, flat.T).astype(BF)

    def body(i, carry):
        for j in range(3):
            for k in range(3):
                rhs = jnp.concatenate(
                    [across_ref[k, t + 2 - i, (2 - j) * W : (4 - j) * W] for t in range(FRAMES)], axis=0
                )
                product = jnp.dot(turn_ref[...], rhs, preferred_element_type=F32)
                put_tap(keep_ref, send_ref, i * 9 + j * 3 + k, product)
        return carry

    lax.fori_loop(0, 3, body, 0)


def first_grad_kernel(
    core_ref, grad_ref, own_ref, rows_ref, time_ref, keep_ref, send_ref, ext_ref, across_ref, turn_ref
):
    core = core_ref[0]
    fill_ext(ext_ref, own_ref, rows_ref, time_ref, 2, 0)
    for t in range(FRAMES):
        for k, copy in enumerate(shift_copies(grad_ref[t].reshape(2 * W, C))):
            across_ref[k, t * 2 * W : (t + 1) * 2 * W] = copy
    for f in range(EXT):
        turn_ref[f] = keep_first(core, ext_ref[f].astype(F32).T).astype(BF)

    def body(i, carry):
        for j in range(3):
            lhs = jnp.concatenate(
                [turn_ref[t + i, :, j * W : (j + 2) * W] for t in range(FRAMES)], axis=1
            )
            for k in range(3):
                product = jnp.dot(lhs, across_ref[k], preferred_element_type=F32)
                put_tap(keep_ref, send_ref, i * 9 + j * 3 + k, product)
        return carry

    lax.fori_loop(0, 3, body, 0)


def cost(flops, moved):
    return pl.CostEstimate(flops=flops, bytes_accessed=moved, transcendentals=0)


def whole(kernel, outs, scratch, limit, smem=0, hbm=(), flops=PASS_FLOPS):
    def call(*args):
        moved = sum(a.size * a.dtype.itemsize for a in args)
        moved += sum(o.size * o.dtype.itemsize for o in outs)
        spaces = [
            pltpu.SMEM if n < smem else pltpu.HBM if n in hbm else pltpu.VMEM for n in range(len(args))
        ]
        return pl.pallas_call(
            kernel,
            out_shape=outs,
            in_specs=[pl.BlockSpec(memory_space=space) for space in spaces],
            out_specs=[pl.BlockSpec(memory_space=pltpu.VMEM) for _ in outs],
            scratch_shapes=scratch,
            compiler_params=pltpu.CompilerParams(vmem_limit_bytes=limit << 20),
            cost_estimate=cost(flops, moved),
        )(*args)

    return call


def convolution(kernel, outs):
    scratch = [
        pltpu.VMEM((EXT, 4 * W, C), BF),
        pltpu.VMEM((3, 9, C, C), BF),
        pltpu.SemaphoreType.DMA((3,)),
    ]
    return whole(kernel, outs, scratch, 24, hbm=(3,))


STEP = 3


def assemble_kernel(core_ref, own_ref, far_ref, first_ref, second_ref):
    core = core_ref[0]
    start = pl.program_id(0) * STEP
    mine = pl.multiple_of(core * 128, 128)
    theirs = pl.multiple_of((1 - core) * 128, 128)
    for grad, out in ((0, second_ref), (1, first_ref)):
        for p in range(STEP):
            for b in range(2):
                lanes = slice(b * 128, (b + 1) * 128)
                for rows, ref in ((mine, own_ref), (theirs, far_ref)):
                    half = ref[grad, :, b, start + p].astype(F32)
                    out[p, pl.ds(rows, 128), lanes] = half.reshape(128, 128)


def assemble(core, own, far):
    own, far = (v.reshape(2, 16, 2, TAPS, 8, 128) for v in (own, far))
    out = pl.BlockSpec((STEP, C, C), lambda p: (p, 0, 0))
    shape = jax.ShapeDtypeStruct((TAPS, C, C), F32)
    whole_array = pl.BlockSpec(memory_space=pltpu.VMEM)
    return pl.pallas_call(
        assemble_kernel,
        out_shape=(shape, shape),
        grid=(TAPS // STEP,),
        in_specs=[pl.BlockSpec(memory_space=pltpu.SMEM), whole_array, whole_array],
        out_specs=(out, out),
        compiler_params=pltpu.CompilerParams(vmem_limit_bytes=24 << 20),
        cost_estimate=cost(1 << 24, 28 << 20),
        name="assemble",
    )(core, own, far)


def total_kernel(parts_ref, out_ref):
    def body(q, carry):
        value = parts_ref[0, q].astype(F32)
        for n in range(1, parts_ref.shape[0]):
            value = value + parts_ref[n, q].astype(F32)
        rounded = value.astype(BF)
        for n in range(out_ref.shape[0]):
            out_ref[n, q] = rounded
        return carry

    lax.fori_loop(0, parts_ref.shape[1], body, 0)


def total(parts, copies):
    shape = jax.ShapeDtypeStruct((copies, *parts.shape[1:]), BF)
    return whole(total_kernel, (shape,), [], 16, flops=1 << 28)(parts)[0]


def stage_groups():
    sizes = [lax.axis_size(axis) for axis in ALL]
    grid = np.arange(math.prod(sizes)).reshape(sizes)
    near, rest = ([], [])
    for core, axis in ((0, 3), (1, 2)):
        chips = np.moveaxis(grid[:, core], axis, -1)
        lines = chips.reshape(-1, chips.shape[-1])
        near += lines.tolist()
        rest += lines.T.tolist()
    return near, rest


def exchange(value, groups):
    return lax.all_to_all(value, ALL, 0, 0, axis_index_groups=groups, tiled=False)


def swap(value, axis, steps):
    count = lax.axis_size(axis)
    pairs = [(n, n + steps) for n in range(count) if 0 <= n + steps < count]
    return lax.ppermute(value, axis, pairs)


def edge_rows(one, two):
    to_above = jnp.stack([one[:, 0], two[:, 0]])
    to_below = jnp.stack([one[:, 1], two[:, 1]])
    above = swap(to_below, SPACE, 1)
    below = swap(to_above, SPACE, -1)
    return jnp.stack([above, below])


def two_frames(own, rows, which, start):
    frames = slice(start, start + 2)
    return jnp.concatenate(
        [rows[0, which, frames][:, None], own[frames], rows[1, which, frames][:, None]], axis=1
    )


def step(latents, first_kernel, second_kernel, upstream):
    core = lax.axis_index("co").astype(jnp.int32).reshape(1)
    k1 = first_kernel.reshape(9, 3, C, C)
    k2 = second_kernel.reshape(9, 3, C, C)
    wide = latents.astype(F32)
    smooth = (wide * jax.nn.sigmoid(wide)).astype(BF)
    block = jax.ShapeDtypeStruct((FRAMES, 2, W, C), BF)
    ext = pltpu.VMEM((EXT, 4 * W, C), BF)

    rows = edge_rows(smooth, upstream)
    smooth_time = swap(two_frames(smooth, rows, 0, 2), GROUP, 1)
    up_time = swap(two_frames(upstream, rows, 1, 0), GROUP, -1)
    hidden, active = convolution(
        hidden_kernel, (jax.ShapeDtypeStruct((FRAMES, 2 * W, C), F32), block)
    )(smooth, rows, smooth_time, pltpu.with_memory_space_constraint(k1, pltpu.HBM))
    (hidden_grad,) = convolution(hidden_grad_kernel, (block,))(
        upstream, rows, up_time, k2, hidden
    )

    late = edge_rows(active, hidden_grad)
    active_time = swap(two_frames(active, late, 0, 2), GROUP, 1)
    grad_time = swap(two_frames(hidden_grad, late, 1, 0), GROUP, -1)

    half = (16, 2, TAPS, 8, 128)
    pair = (jax.ShapeDtypeStruct(half, F32), jax.ShapeDtypeStruct(half, BF))
    keep2, send2 = whole(
        second_grad_kernel, pair, [ext, pltpu.VMEM((3, EXT, 4 * W, C), BF), pltpu.VMEM((C, FRAMES * 2 * W), BF)], 40, 1
    )(core, active, upstream, rows, up_time)
    keep1, send1 = whole(
        first_grad_kernel, pair, [ext, pltpu.VMEM((3, FRAMES * 2 * W, C), BF), pltpu.VMEM((EXT, C, 4 * W), BF)], 40, 1
    )(core, hidden_grad, smooth, rows, smooth_time)

    across = [(0, 1), (1, 0)]
    got2 = lax.ppermute(send2, "co", across)
    got1 = lax.ppermute(send1, "co", across)
    mine = jnp.stack([(keep2 + got2.astype(F32)).astype(BF), (keep1 + got1.astype(F32)).astype(BF)])
    near, rest = stage_groups()
    first, second = (len(near[0]), len(rest[0]))
    block_rows = 64 // (first * second) * TAPS
    parts = exchange(mine.reshape(first, second, block_rows, 8, 128), near)
    quarter = total(parts, 1)
    parts = exchange(quarter.reshape(second, block_rows, 8, 128), rest)
    spread = total(parts[:, None], second)
    quarter = exchange(spread.reshape(second, block_rows, 8, 128), rest)
    own = exchange(jnp.broadcast_to(quarter[None], (first, *quarter.shape)), near)
    far = lax.ppermute(own, "co", across)

    (decoded,) = convolution(decoded_kernel, (block,))(
        active, late, active_time, k2, latents
    )
    (latent_grad,) = convolution(latent_grad_kernel, (block,))(hidden_grad, late, grad_time, k1, latents, upstream)
    first_grad, second_grad = assemble(core, own, far)
    shape = first_kernel.shape
    return (decoded, latent_grad, first_grad.reshape(shape), second_grad.reshape(shape))


def solution(mesh, sizes=(2, 2, 2, 4, 4)):
    fine = Mesh(mesh.devices.reshape(sizes), ("zl", "co", "zh", "y", "x"))
    placed = (P(GROUP, SPACE, None, None), P(), P(), P(GROUP, SPACE, None, None))
    return jax.shard_map(
        step,
        mesh=fine,
        in_specs=placed,
        out_specs=(P(GROUP, SPACE, None, None), P(GROUP, SPACE, None, None), P(), P()),
        check_vma=False,
    )
```
